32 devices in a mesh: groups: 2 (over x), row: 16 (over z, y, core).
Axes of the slice: x: 2, y: 2, z: 4, core: 2. Of those that a mesh axis runs over, the one named last changes fastest.
Arguments:
- factor_b: bfloat16 [64, 131072], P(None, ('groups', 'row')), parts along dimension 1, may hold values from -12 to 12
- factor_c: bfloat16 [64, 131072], P(None, ('groups', 'row')), parts along dimension 1, may hold values from -12 to 12
- sample_j: int32 [262144], P(('groups', 'row')), parts along dimension 0, may hold values from 0 to 65535, as said below
- sample_k: int32 [16, 32, 512], P(None, ('groups', 'row')), parts along dimension 1, may hold values from 0 to 65535, as said below
- sample_weight: float32 [262144], P(('groups', 'row')), parts along dimension 0, may hold values from 0.5 to 3.5
- block_values: bfloat16 [32, 16, 4, 4, 128], P(('groups', 'row')), parts along dimension 0, may hold values from -24 to 24
- block_sample: int32 [32, 16, 4, 4], P(('groups', 'row')), parts along dimension 0, may hold values from 0 to 8191
- block_count: int32 [32, 16, 4, 4], P(('groups', 'row')), parts along dimension 0, may hold values from 0 to 128, as said below
Outputs:
- factor_new: bfloat16 [64, 16384], P(None, ('groups', 'row')), parts along dimension 1
- scales: float32 [128], P('groups'), parts along dimension 0
The draws below stay inside these ranges and needn't reach their ends.
There are 2 independent parts, one for each index of `groups`. The reference program is written for one: setup_inputs(seed, part) draws one part's arguments, and reference() takes and returns one part's arrays. A program takes and returns all parts, laid end to end along the dimension named above; each array names one. Nothing has to cross between parts.
Inputs may be any that keep to these rules, and one draw needn't show every extreme that they name: sample_j[s] lies in rows s // 8192 * 4096 to s // 8192 * 4096 + 4095. sample_k[d, e, i] is the third-mode index of sample d * 8192 + e * 512 + i and lies in rows e * 4096 to e * 4096 + 4095. `block_count`: 0 marks an empty slot; slot [p, p, 0, 0] holds 128 for every p.
All inputs are finite; a program needn't handle non-finite values.
Results may differ from the reference program's by a relative error of at most 0.0051.
Values may be sent and summed in bfloat16 or wider, within the bound.
A program may use at most 64 MiB of HBM per device.

```python
import math
import jax
import jax.numpy as jnp
from jax import lax

R = 64
JD = 4096
KD = 4096
S_DEV = 8192
TD = 4
CT = 4
SPN = 512
S = 131072
J = 65536
K = 65536
I = 8192
N_ROW = 16


def factor_draw(key, total_rows):
    key_scale = jax.random.fold_in(key, 11)
    key_own = jax.random.fold_in(key, 12)
    key_spread = jax.random.fold_in(key, 14)
    column_scale = jnp.exp(jax.random.uniform(key_scale, (R, 1), minval=-math.log(1.5), maxval=math.log(1.5)))
    heavy_column = jax.random.randint(key_spread, (1, total_rows), 0, 128, dtype=jnp.int32) == 0
    spread_factor = jnp.where(heavy_column, 5.5, 0.8).astype(jnp.float32)
    own_part = jax.random.normal(key_own, (R, total_rows), dtype=jnp.float32)
    return (jnp.clip(own_part * spread_factor, -8.0, 8.0) * column_scale).astype(jnp.bfloat16)


def draw_factor_b(key, part):
    return factor_draw(jax.random.fold_in(key, 1), J)


def draw_factor_c(key, part):
    return factor_draw(jax.random.fold_in(key, 2), K)


def draw_sample_j(key, part):
    owner_block = jnp.arange(S, dtype=jnp.int32) // S_DEV
    offsets = jax.random.randint(jax.random.fold_in(key, 3), (S,), 0, JD, dtype=jnp.int32)
    return owner_block * JD + offsets


def draw_sample_k(key, part):
    holder = lax.broadcasted_iota(jnp.int32, (N_ROW, N_ROW, SPN), 1)
    offsets = jax.random.randint(jax.random.fold_in(key, 4), (N_ROW, N_ROW, SPN), 0, KD, dtype=jnp.int32)
    return holder * KD + offsets


def draw_sample_weight(key, part):
    device_pos = (jnp.arange(S, dtype=jnp.int32) // S_DEV).astype(jnp.float32)
    lift = jnp.sqrt(1.0 + 2.0 * device_pos / (N_ROW - 1))
    key_base = jax.random.fold_in(key, 5)
    base_weight = jnp.exp(jax.random.uniform(key_base, (S,), minval=-math.log(2.0), maxval=math.log(2.0)))
    return base_weight * lift


def draw_block_values(key, part):
    slot_shape = (N_ROW, N_ROW, TD, CT, 128)
    target = lax.broadcasted_iota(jnp.int32, slot_shape, 1).astype(jnp.float32)
    target_scale = 1.0 + 2.0 * target / (N_ROW - 1)
    key_noise = jax.random.fold_in(key, 6)
    noise_field = jax.random.normal(key_noise, slot_shape, dtype=jnp.float32)
    return (jnp.clip(noise_field, -8.0, 8.0) * target_scale).astype(jnp.bfloat16)


def draw_block_count(key, part):
    slot_shape = (N_ROW, N_ROW, TD, CT)
    source_ids = lax.broadcasted_iota(jnp.int32, slot_shape, 0)
    target_ids = lax.broadcasted_iota(jnp.int32, slot_shape, 1)
    tile_ids = lax.broadcasted_iota(jnp.int32, slot_shape, 2)
    slot_ids = lax.broadcasted_iota(jnp.int32, slot_shape, 3)
    fill_level = jax.random.randint(jax.random.fold_in(key, 7), (N_ROW,), 5, 9, dtype=jnp.int32)
    live_slot = jax.random.randint(jax.random.fold_in(key, 8), slot_shape, 0, 8, dtype=jnp.int32) < fill_level[None, :, None, None]
    most_live = 43 + 85 * source_ids // (N_ROW - 1)
    least_live = most_live // 2
    raw_count = jax.random.randint(jax.random.fold_in(key, 9), slot_shape, 0, 1 << 20, dtype=jnp.int32) % (most_live - least_live) + least_live + 1
    counted = jnp.where(live_slot, raw_count, jnp.zeros_like(raw_count))
    fixed_slot = (source_ids == target_ids) & (tile_ids == 0) & (slot_ids == 0)
    return jnp.where(fixed_slot, jnp.full_like(counted, 128), counted)


def place_ends(drawn, own_key, smallest, top_value):
    place = [jax.random.randint(jax.random.fold_in(own_key, axis), (), 0, length) for axis, length in enumerate(drawn.shape)]
    main_axis = drawn.shape.index(max(drawn.shape))
    beside = place[:main_axis] + [(place[main_axis] + 1) % drawn.shape[main_axis]] + place[main_axis + 1:]
    return drawn.at[tuple(place)].set(smallest).at[tuple(beside)].set(top_value)


def setup_inputs(seed: int = 0, part: int = 0) -> dict:
    key_list = jax.random.split(jax.random.key(seed), 9)
    own_keys = jax.random.split(jax.random.fold_in(key_list[8], part), 9)
    return {
        "factor_b": draw_factor_b(jax.random.fold_in(jax.random.fold_in(key_list[8], part), 71), part),
        "factor_c": draw_factor_c(jax.random.fold_in(jax.random.fold_in(key_list[8], part), 71), part),
        "sample_j": draw_sample_j(jax.random.fold_in(jax.random.fold_in(key_list[8], part), 71), part),
        "sample_k": draw_sample_k(jax.random.fold_in(jax.random.fold_in(key_list[8], part), 71), part),
        "sample_weight": draw_sample_weight(jax.random.fold_in(jax.random.fold_in(key_list[8], part), 71), part),
        "block_values": draw_block_values(jax.random.fold_in(jax.random.fold_in(key_list[8], part), 71), part),
        "block_sample": place_ends(jax.random.randint(own_keys[6], (N_ROW, N_ROW, TD, CT), 0, S_DEV), jax.random.fold_in(own_keys[6], 1), 0, S_DEV - 1).astype(jnp.int32),
        "block_count": draw_block_count(jax.random.fold_in(jax.random.fold_in(key_list[8], part), 71), part),
    }


def reference(factor_b, factor_c, sample_j, sample_k, sample_weight, block_values, block_sample, block_count):
    rank_width = factor_b.shape[0]
    b_columns = jnp.take(factor_b, sample_j, axis=1).astype(jnp.float32)
    c_columns = jnp.take(factor_c, sample_k.reshape(-1), axis=1).astype(jnp.float32)
    sketch = sample_weight[None, :] * b_columns * c_columns
    gram_matrix = jnp.dot(sketch, sketch.T, precision=lax.Precision.HIGHEST)
    live_total = jnp.sum(block_count.astype(jnp.float32))
    ridge = 0.05 * live_total / I
    system = gram_matrix / S + ridge * jnp.eye(rank_width, dtype=jnp.float32)
    lower_factor = jnp.linalg.cholesky(system)
    weighted = (sample_weight[None, :] * sketch).astype(jnp.bfloat16)
    positions = lax.broadcasted_iota(jnp.int32, block_values.shape, 4)
    masked = jnp.where(positions < block_count[..., None], block_values, jnp.zeros_like(block_values))
    owners = lax.broadcasted_iota(jnp.int32, block_sample.shape, 0) * S_DEV + block_sample
    picked = jnp.take(weighted, owners.reshape(-1).astype(jnp.int32), axis=1)
    picked = picked.reshape((rank_width,) + block_sample.shape)
    gathered = jnp.einsum('pqtcr,kpqtc->kqtr', masked.astype(jnp.float32), picked.astype(jnp.float32), precision=lax.Precision.HIGHEST).reshape(rank_width, -1)
    half_solved = lax.linalg.triangular_solve(lower_factor, gathered, left_side=True, lower=True)
    update = lax.linalg.triangular_solve(lower_factor, half_solved, left_side=True, lower=True, transpose_a=True)
    column_sums = lax.optimization_barrier(jnp.sum(update * update, axis=1))
    scales = jnp.sqrt(column_sums / I + 1e-06)
    return ((update / scales[:, None]).astype(jnp.bfloat16), scales)
```

```python
import functools

import jax
import jax.numpy as jnp
from jax import lax
from jax.experimental import pallas as pl
from jax.experimental.pallas import tpu as pltpu
from jax.sharding import PartitionSpec as P

NT = (((1,), (1,)), ((), ()))
TN = (((0,), (0,)), ((), ()))
MESH = pl.DeviceIdType.MESH
UNROLLED_PEERS = 16
PANEL = 4


def pick_columns(folded, index, rank):
    width = folded.shape[1]
    count = index.shape[1]
    low = lax.rem(index, width)
    high = lax.div(index, width)
    rows = lax.broadcasted_iota(jnp.int16, (width, count), 0)
    one_hot = jnp.where(rows == low.astype(jnp.int16), jnp.bfloat16(1), jnp.bfloat16(0))
    products = jnp.dot(folded[...], one_hot, preferred_element_type=jnp.float32)
    picked = products[:rank]
    high = jnp.broadcast_to(high, (rank, count))
    for part in range(1, folded.shape[0] // rank):
        picked = jnp.where(high == part, products[part * rank : (part + 1) * rank], picked)
    return picked


def block_column(table_ref):
    table = jnp.concatenate([table_ref[tile] for tile in range(table_ref.shape[0])], axis=0)
    return jnp.concatenate(
        [table[:, peer : peer + 1] for peer in range(table.shape[1])], axis=0
    )


def inverse(matrix):
    order = matrix.shape[0]
    lanes = lax.broadcasted_iota(jnp.int32, (1, order), 1)
    rows = lax.broadcasted_iota(jnp.int32, (order, 1), 0)
    for first in range(0, order, PANEL):
        panel = [
            jnp.broadcast_to(matrix[:, k : k + 1], matrix.shape)
            for k in range(first, first + PANEL)
        ]
        for step in range(PANEL):
            k = first + step
            column = panel[step]
            pivot = 1.0 / column[k : k + 1, :]
            scaled = jnp.where(lanes == k, 1.0, matrix[k : k + 1, :]) * pivot
            own = rows == k
            matrix = jnp.where(
                own, scaled, jnp.where(lanes == k, 0.0, matrix) - column * scaled
            )
            for later in range(step + 1, PANEL):
                factor = panel[later][k : k + 1, :] * pivot
                panel[later] = jnp.where(own, factor, panel[later] - column * factor)
    return matrix


def kernel(
    n,
    tiles,
    slots,
    total_rows,
    total_samples,
    b_hbm,
    c_hbm,
    j_hbm,
    k_hbm,
    w_hbm,
    values_hbm,
    sample_hbm,
    count_hbm,
    out_ref,
    scales_ref,
    folded_b,
    folded_c,
    j_ref,
    k_ref,
    w_ref,
    values_ref,
    sample_ref,
    count_ref,
    c_out,
    c_in,
    b_weighted,
    values_out,
    values_in,
    spread_ref,
    picks_out,
    picks_in,
    gram_out,
    gram_in,
    share_out,
    share_in,
    sample_column,
    sums_out,
    sums_in,
    load_sems,
    c_send,
    c_recv,
    send_sems,
    recv_sems,
):
    me = lax.axis_index("row")
    rank, b_rows = b_hbm.shape
    c_rows = c_hbm.shape[1]
    width = folded_c.shape[1]
    per_peer = tiles * slots
    blocks = n * per_peer
    chunk = c_in.shape[2]
    half = n // 2
    side = me // half
    place = me % half

    def far(turn):
        return (1 - side) * half + (place + turn) % half

    def near(turn):
        return side * half + (place + turn) % half

    def loop(start, stop, body):
        if n <= UNROLLED_PEERS:
            for turn in range(start, stop):
                body(turn)
        else:
            lax.fori_loop(start, stop, lambda turn, carry: (body(turn), carry)[1], 0)

    def each_peer(body):
        loop(0, half, lambda turn: body(far(turn)))
        loop(1, half, lambda turn: body(near(turn)))

    def remote(peer, source, target, send, recv):
        return pltpu.make_async_remote_copy(
            src_ref=source,
            dst_ref=target,
            send_sem=send,
            recv_sem=recv,
            device_id={"row": peer},
            device_id_type=MESH,
        )

    def copy_c(peer, slot):
        return remote(peer, c_out.at[peer], c_in.at[slot], c_send.at[peer], c_recv.at[slot])

    def others(kind, target):
        region = target.at[pl.ds(0, n - 1)]
        return remote(near(1), region, region, send_sems.at[kind], recv_sems.at[kind])

    barrier = pltpu.get_barrier_semaphore()
    each_peer(
        lambda peer: pl.semaphore_signal(
            barrier, inc=1, device_id={"row": peer}, device_id_type=MESH
        )
    )

    def load_table(source, target, kind):
        return [
            pltpu.make_async_copy(
                source.at[:, pl.ds(part * width, width)],
                target.at[pl.ds(part * rank, rank)],
                load_sems.at[kind],
            )
            for part in range(source.shape[1] // width)
        ]

    load_c = load_table(c_hbm, folded_c, 0)
    load_b = load_table(b_hbm, folded_b, 1)
    load_k = pltpu.make_async_copy(k_hbm, k_ref, load_sems.at[2])
    load_j = pltpu.make_async_copy(j_hbm, j_ref, load_sems.at[3])
    load_w = pltpu.make_async_copy(w_hbm, w_ref, load_sems.at[4])
    load_values = pltpu.make_async_copy(values_hbm, values_ref, load_sems.at[5])
    load_sample = pltpu.make_async_copy(sample_hbm, sample_ref, load_sems.at[6])
    load_count = pltpu.make_async_copy(count_hbm, count_ref, load_sems.at[7])
    for load in [load_k, *load_c, load_count, load_values, load_sample, load_j, *load_b, load_w]:
        load.start()

    def pick_c(peer):
        return pick_columns(folded_c, k_ref[peer] - me * c_rows, rank).astype(jnp.bfloat16)

    load_k.wait()
    for load in load_c:
        load.wait()
    c_out[far(0)] = pick_c(far(0))
    load_count.wait()
    load_values.wait()
    lanes = lax.broadcasted_iota(jnp.int32, (blocks, 128), 1)
    counts = block_column(count_ref)
    live = lanes < counts
    masked = jnp.where(live, values_ref[...].astype(jnp.float32), 0.0).astype(jnp.bfloat16)
    values_out[...] = masked.reshape(values_out.shape)
    values_in[me] = values_out[me]
    live_local = jnp.sum(counts.astype(jnp.float32), axis=0, keepdims=True)
    pl.semaphore_wait(barrier, n - 1)
    copy_c(far(0), me).start()
    each_peer(
        lambda peer: remote(
            peer, values_out.at[peer], values_in.at[me], send_sems.at[0], recv_sems.at[0]
        ).start()
    )

    def send_c(peer):
        c_out[peer] = pick_c(peer)
        copy_c(peer, me).start()

    def send_far(turn, carry):
        send_c(far(turn))
        return carry

    def send_near(turn, carry):
        send_c(near(turn))
        return carry

    lax.fori_loop(1, half, send_far, 0)
    lax.fori_loop(1, half, send_near, 0)
    c_in[me] = pick_c(me)
    load_j.wait()
    load_w.wait()
    load_sample.wait()
    for load in load_b:
        load.wait()

    def pick_b(part, carry):
        picked = pick_columns(folded_b, j_ref[part] - me * b_rows, rank)
        b_weighted[part] = w_ref[part] * picked
        return carry

    lax.fori_loop(0, n, pick_b, 0)
    columns = lax.broadcasted_iota(jnp.int32, (blocks, chunk), 1)
    sample_column[...] = block_column(sample_ref)

    def add_chunk(part, carry):
        gram, picks = carry
        weights = w_ref[part]
        sketch = b_weighted[part] * c_in[part].astype(jnp.float32)
        top = sketch.astype(jnp.bfloat16)
        rest = (sketch - top.astype(jnp.float32)).astype(jnp.bfloat16)
        both = jnp.concatenate([top, rest], axis=0)
        gram = gram + lax.dot_general(both, both, NT, preferred_element_type=jnp.float32)
        weighted = (weights * sketch).astype(jnp.bfloat16)
        chosen = columns == sample_column[...] - part * chunk
        chosen = jnp.where(chosen, 1.0, 0.0).astype(jnp.bfloat16)
        picks = picks + lax.dot_general(
            chosen, weighted, NT, preferred_element_type=jnp.float32
        )
        return gram, picks

    def add_peer(part, carry):
        copy_c(part, part).wait_recv()
        return add_chunk(part, carry)

    carry = (
        jnp.zeros((2 * rank, 2 * rank), jnp.float32),
        jnp.zeros((blocks, rank), jnp.float32),
    )
    carry = add_chunk(me, carry)
    carry = lax.fori_loop(1, half, lambda turn, carry: add_peer(near(turn), carry), carry)

    others(0, values_in).wait_recv()
    arrived = values_in[...].astype(jnp.float32)
    rows_half = per_peer // 2
    tile_of = lax.broadcasted_iota(jnp.int32, (n * rows_half, 128), 0) % rows_half // slots
    for part in range(2):
        rows = arrived[:, part * rows_half : (part + 1) * rows_half, :].reshape(-1, 128)
        spread_ref[part] = jnp.concatenate(
            [jnp.where(tile_of == tile, rows, 0.0) for tile in range(tiles // 2)], axis=1
        ).astype(jnp.bfloat16)

    gram, picks = lax.fori_loop(
        0,
        half,
        lambda turn, carry: add_peer(side * turn + (1 - side) * (n - 1 - turn), carry),
        carry,
    )

    pair = gram[:rank] + gram[rank:]
    pair = (pair + pltpu.roll(pair, rank, 1)) / total_samples
    pair_rows = lax.broadcasted_iota(jnp.int32, pair.shape, 0)
    pair_lanes = lax.broadcasted_iota(jnp.int32, pair.shape, 1)
    ridge = 0.05 * live_local / total_rows
    pair = pair + jnp.where(pair_lanes % rank == pair_rows, ridge, 0.0)
    fold = rank // (n * gram_out.shape[1])
    if fold == 2:
        first_half = lax.broadcasted_iota(jnp.int32, (rank // 2, 2 * rank), 1) < rank
        pair = jnp.where(first_half, pair[: rank // 2], pair[rank // 2 :])
    piece = gram_out.shape[1]
    for part in range(n):
        gram_out[part] = pair[part * piece : (part + 1) * piece]
    gram_in[me] = gram_out[me]
    each_peer(
        lambda peer: remote(
            peer, gram_out.at[peer], gram_in.at[me], send_sems.at[1], recv_sems.at[1]
        ).start()
    )
    picks = picks.reshape(n, per_peer, rank)
    picks_out[...] = jnp.concatenate(
        [picks[:, :rows_half], picks[:, rows_half:]], axis=2
    ).astype(jnp.bfloat16)
    picks_in[me] = picks_out[me]
    each_peer(
        lambda peer: remote(
            peer, picks_out.at[peer], picks_in.at[me], send_sems.at[2], recv_sems.at[2]
        ).start()
    )
    others(1, gram_in).wait_recv()
    share_out[...] = jnp.sum(gram_in[...], axis=0)
    share_in[me] = share_out[...]
    each_peer(
        lambda peer: remote(
            peer, share_out, share_in.at[me], send_sems.at[3], recv_sems.at[3]
        ).start()
    )
    others(2, picks_in).wait_recv()
    arrived = picks_in[...].astype(jnp.float32).reshape(-1, 2 * rank).astype(jnp.bfloat16)
    gathered = jnp.concatenate(
        [
            lax.dot_general(arrived, spread_ref[part], TN, preferred_element_type=jnp.float32)[
                part * rank : (part + 1) * rank
            ]
            for part in range(2)
        ],
        axis=1,
    )
    others(3, share_in).wait_recv()
    total = jnp.concatenate([share_in[part] for part in range(n)], axis=0)
    if fold == 2:
        total = jnp.concatenate([total[:, :rank], total[:, rank:]], axis=0)
    else:
        total = total[:, :rank]
    inverted = inverse(total)
    update = jnp.dot(
        inverted,
        gathered,
        precision=lax.Precision.HIGHEST,
        preferred_element_type=jnp.float32,
    )
    gram_rows = lax.broadcasted_iota(jnp.int32, (rank, rank), 0)
    diagonal = gram_rows == lax.broadcasted_iota(jnp.int32, (rank, rank), 1)
    squares = jnp.sum(update * update, axis=1, keepdims=True)
    squares = jnp.sum(jnp.where(diagonal, squares, 0.0), axis=0, keepdims=True)
    sums_out[...] = jnp.concatenate([squares, jnp.zeros_like(squares)], axis=1)
    sums_in[me] = sums_out[...]
    each_peer(
        lambda peer: remote(
            peer, sums_out, sums_in.at[me], send_sems.at[4], recv_sems.at[4]
        ).start()
    )
    others(4, sums_in).wait_recv()
    sums = jnp.sum(sums_in[...], axis=0)
    scales = jnp.sqrt(sums[:, :rank] / total_rows + 1e-06)
    scales_ref[...] = scales
    scale_column = jnp.sum(jnp.where(diagonal, scales, 0.0), axis=1, keepdims=True)
    out_ref[...] = (update / scale_column).astype(out_ref.dtype)

    each_peer(lambda peer: copy_c(peer, me).wait_send())
    others(0, values_out).wait_send()
    others(1, gram_out).wait_send()
    others(2, picks_out).wait_send()
    others(3, share_in).wait_send()
    others(4, sums_in).wait_send()


def shards(
    factor_b, factor_c, sample_j, sample_k, sample_weight, block_values, block_sample, block_count
):
    rank, b_rows = factor_b.shape
    n, _, chunk = sample_k.shape
    _, _, tiles, slots, tile_rows = block_values.shape
    samples = sample_j.shape[0]
    per_peer = tiles * slots
    blocks = n * per_peer
    width = 512
    piece = max(rank // (2 * n), 1)
    bf16, f32, i32 = jnp.bfloat16, jnp.float32, jnp.int32
    hbm = pl.BlockSpec(memory_space=pltpu.HBM)
    vmem = pl.BlockSpec(memory_space=pltpu.VMEM)
    factor_new, scales = pl.pallas_call(
        functools.partial(kernel, n, tiles, slots, tiles * tile_rows * n, samples * n),
        out_shape=(
            pltpu.VMEM((rank, tiles * tile_rows), bf16),
            pltpu.VMEM((1, rank), f32),
        ),
        in_specs=[hbm] * 8,
        out_specs=(vmem, vmem),
        scratch_shapes=[
            pltpu.VMEM((b_rows // width * rank, width), bf16),
            pltpu.VMEM((factor_c.shape[1] // width * rank, width), bf16),
            pltpu.VMEM((n, 1, chunk), i32),
            pltpu.VMEM((n, 1, chunk), i32),
            pltpu.VMEM((n, 1, chunk), f32),
            pltpu.VMEM((blocks, tile_rows), bf16),
            pltpu.VMEM((tiles, slots, n), i32),
            pltpu.VMEM((tiles, slots, n), i32),
            pltpu.VMEM((n, rank, chunk), bf16),
            pltpu.VMEM((n, rank, chunk), bf16),
            pltpu.VMEM((n, rank, chunk), f32),
            pltpu.VMEM((n, per_peer, tile_rows), bf16),
            pltpu.VMEM((n, per_peer, tile_rows), bf16),
            pltpu.VMEM((2, blocks // 2, tiles // 2 * tile_rows), bf16),
            pltpu.VMEM((n, per_peer // 2, 2 * rank), bf16),
            pltpu.VMEM((n, per_peer // 2, 2 * rank), bf16),
            pltpu.VMEM((n, piece, 2 * rank), f32),
            pltpu.VMEM((n, piece, 2 * rank), f32),
            pltpu.VMEM((piece, 2 * rank), f32),
            pltpu.VMEM((n, piece, 2 * rank), f32),
            pltpu.VMEM((blocks, 1), i32),
            pltpu.VMEM((1, 2 * rank), f32),
            pltpu.VMEM((n, 1, 2 * rank), f32),
            pltpu.SemaphoreType.DMA((8,)),
            pltpu.SemaphoreType.DMA((n,)),
            pltpu.SemaphoreType.DMA((n,)),
            pltpu.SemaphoreType.DMA((5,)),
            pltpu.SemaphoreType.DMA((5,)),
        ],
        compiler_params=pltpu.CompilerParams(collective_id=0, has_side_effects=True),
    )(
        factor_b,
        factor_c,
        sample_j.reshape(n, 1, chunk),
        sample_k,
        sample_weight.reshape(n, 1, chunk),
        block_values.reshape(blocks, tile_rows),
        block_sample[0].transpose(1, 2, 0),
        block_count[0].transpose(1, 2, 0),
    )
    return factor_new, scales.reshape(rank)


def solution(mesh):
    in_specs = (
        P(None, ("groups", "row")),
        P(None, ("groups", "row")),
        P(("groups", "row")),
        P(None, ("groups", "row"), None),
        P(("groups", "row")),
        P(("groups", "row"), None, None, None, None),
        P(("groups", "row"), None, None, None),
        P(("groups", "row"), None, None, None),
    )
    out_specs = (P(None, ("groups", "row")), P("groups"))
    return jax.shard_map(shards, mesh=mesh, in_specs=in_specs, out_specs=out_specs, check_vma=False)
```

```python
import functools

import jax
import jax.numpy as jnp
from jax import lax
from jax.experimental import pallas as pl
from jax.experimental.pallas import tpu as pltpu
from jax.sharding import PartitionSpec as P

NT = (((1,), (1,)), ((), ()))
TN = (((0,), (0,)), ((), ()))
MESH = pl.DeviceIdType.MESH
UNROLLED_PEERS = 16
PANEL = 4


def pick_columns(folded, index, rank):
    width = folded.shape[1]
    count = index.shape[1]
    low = lax.rem(index, width)
    high = lax.div(index, width)
    rows = lax.broadcasted_iota(jnp.int16, (width, count), 0)
    one_hot = jnp.where(rows == low.astype(jnp.int16), jnp.bfloat16(1), jnp.bfloat16(0))
    products = jnp.dot(folded[...], one_hot, preferred_element_type=jnp.float32)
    picked = products[:rank]
    high = jnp.broadcast_to(high, (rank, count))
    for part in range(1, folded.shape[0] // rank):
        picked = jnp.where(high == part, products[part * rank : (part + 1) * rank], picked)
    return picked


def block_column(table_ref):
    table = jnp.concatenate([table_ref[tile] for tile in range(table_ref.shape[0])], axis=0)
    return jnp.concatenate(
        [table[:, peer : peer + 1] for peer in range(table.shape[1])], axis=0
    )


def inverse(matrix):
    order = matrix.shape[0]
    lanes = lax.broadcasted_iota(jnp.int32, (1, order), 1)
    rows = lax.broadcasted_iota(jnp.int32, (order, 1), 0)
    for first in range(0, order, PANEL):
        panel = [
            jnp.broadcast_to(matrix[:, k : k + 1], matrix.shape)
            for k in range(first, first + PANEL)
        ]
        for step in range(PANEL):
            k = first + step
            column = panel[step]
            pivot = 1.0 / column[k : k + 1, :]
            scaled = jnp.where(lanes == k, 1.0, matrix[k : k + 1, :]) * pivot
            own = rows == k
            matrix = jnp.where(
                own, scaled, jnp.where(lanes == k, 0.0, matrix) - column * scaled
            )
            for later in range(step + 1, PANEL):
                factor = panel[later][k : k + 1, :] * pivot
                panel[later] = jnp.where(own, factor, panel[later] - column * factor)
    return matrix


def kernel(
    n,
    tiles,
    slots,
    total_rows,
    total_samples,
    b_hbm,
    c_hbm,
    j_hbm,
    k_hbm,
    w_hbm,
    values_hbm,
    sample_hbm,
    count_hbm,
    out_ref,
    scales_ref,
    folded_b,
    folded_c,
    j_ref,
    k_ref,
    w_ref,
    values_ref,
    sample_ref,
    count_ref,
    c_out,
    c_in,
    b_weighted,
    values_out,
    values_in,
    spread_ref,
    picks_out,
    picks_in,
    gram_out,
    gram_in,
    share_out,
    share_in,
    sample_column,
    moment_out,
    moment_in,
    moments_out,
    moments_in,
    load_sems,
    c_send,
    c_recv,
    send_sems,
    recv_sems,
):
    me = lax.axis_index("row")
    rank, b_rows = b_hbm.shape
    c_rows = c_hbm.shape[1]
    width = folded_c.shape[1]
    per_peer = tiles * slots
    blocks = n * per_peer
    chunk = c_in.shape[2]
    quarter = n // 4
    own = me // quarter
    place = me % quarter
    side = own // 2
    inner = (own + side) % 2

    def member(frame, turn):
        return (frame + side * (3 - 2 * frame)) * quarter + (place + turn) % quarter

    def sibling(turn):
        return own * quarter + (place + turn) % quarter

    def send_turn(turn):
        block = turn // quarter
        first, last = (2 - block) // 2, block // 2
        frame = first * (2 - 2 * inner) + (1 - first - last) * 3 + last * (1 + inner)
        return member(frame, turn % quarter)

    def late_turn(turn):
        block = turn // quarter
        return member((1 - block) * (3 - 3 * inner) + block * 2, turn % quarter)

    def loop(start, stop, body):
        if n <= UNROLLED_PEERS:
            for turn in range(start, stop):
                body(turn)
        else:
            lax.fori_loop(start, stop, lambda turn, carry: (body(turn), carry)[1], 0)

    def each_peer(body):
        for frame in (3, 2, 1 - inner):
            loop(0, quarter, lambda turn, frame=frame: body(member(frame, turn)))
        loop(1, quarter, lambda turn: body(sibling(turn)))

    def remote(peer, source, target, send, recv):
        return pltpu.make_async_remote_copy(
            src_ref=source,
            dst_ref=target,
            send_sem=send,
            recv_sem=recv,
            device_id={"row": peer},
            device_id_type=MESH,
        )

    def copy_c(peer, slot):
        return remote(peer, c_out.at[peer], c_in.at[slot], c_send.at[peer], c_recv.at[slot])

    def others(kind, target):
        region = target.at[pl.ds(0, n - 1)]
        return remote(sibling(1), region, region, send_sems.at[kind], recv_sems.at[kind])

    def spread_out(source, target, kind):
        each_peer(
            lambda peer: remote(
                peer, source.at[peer], target.at[me], send_sems.at[kind], recv_sems.at[kind]
            ).start()
        )

    piece = gram_out.shape[1]
    fold = rank // (n * piece)

    def scatter(pair, source, target, kind):
        if fold == 2:
            upper = lax.broadcasted_iota(jnp.int32, (rank // 2, 2 * rank), 1) < rank
            pair = jnp.where(upper, pair[: rank // 2], pair[rank // 2 :])
        for part in range(n):
            source[part] = pair[part * piece : (part + 1) * piece]
        target[me] = source[me]
        spread_out(source, target, kind)

    def gather(arrived, source, target, kind):
        source[...] = jnp.sum(arrived[...], axis=0)
        target[me] = source[...]
        each_peer(
            lambda peer: remote(
                peer, source, target.at[me], send_sems.at[kind], recv_sems.at[kind]
            ).start()
        )

    def whole(arrived):
        matrix = jnp.concatenate([arrived[part] for part in range(n)], axis=0)
        if fold == 2:
            return jnp.concatenate([matrix[:, :rank], matrix[:, rank:]], axis=0)
        return matrix[:, :rank]

    barrier = pltpu.get_barrier_semaphore()
    each_peer(
        lambda peer: pl.semaphore_signal(
            barrier, inc=1, device_id={"row": peer}, device_id_type=MESH
        )
    )

    def load_table(source, target, kind):
        return [
            pltpu.make_async_copy(
                source.at[:, pl.ds(part * width, width)],
                target.at[pl.ds(part * rank, rank)],
                load_sems.at[kind],
            )
            for part in range(source.shape[1] // width)
        ]

    load_c = load_table(c_hbm, folded_c, 0)
    load_b = load_table(b_hbm, folded_b, 1)
    load_k = pltpu.make_async_copy(k_hbm, k_ref, load_sems.at[2])
    load_j = pltpu.make_async_copy(j_hbm, j_ref, load_sems.at[3])
    load_w = pltpu.make_async_copy(w_hbm, w_ref, load_sems.at[4])
    load_values = pltpu.make_async_copy(values_hbm, values_ref, load_sems.at[5])
    load_sample = pltpu.make_async_copy(sample_hbm, sample_ref, load_sems.at[6])
    load_count = pltpu.make_async_copy(count_hbm, count_ref, load_sems.at[7])
    for load in [load_k, *load_c, load_count, load_values, load_sample, load_j, *load_b, load_w]:
        load.start()

    def pick_c(peer):
        return pick_columns(folded_c, k_ref[peer] - me * c_rows, rank).astype(jnp.bfloat16)

    load_k.wait()
    for load in load_c:
        load.wait()
    c_out[send_turn(0)] = pick_c(send_turn(0))
    load_count.wait()
    load_values.wait()
    lanes = lax.broadcasted_iota(jnp.int32, (blocks, 128), 1)
    counts = block_column(count_ref)
    live = lanes < counts
    masked = jnp.where(live, values_ref[...].astype(jnp.float32), 0.0).astype(jnp.bfloat16)
    values_out[...] = masked.reshape(values_out.shape)
    values_in[me] = values_out[me]
    live_local = jnp.sum(counts.astype(jnp.float32), axis=0, keepdims=True)
    pl.semaphore_wait(barrier, n - 1)
    copy_c(send_turn(0), me).start()

    def send_c(peer):
        c_out[peer] = pick_c(peer)
        copy_c(peer, me).start()

    def send_far(turn, carry):
        send_c(send_turn(turn))
        return carry

    def send_near(turn, carry):
        send_c(sibling(turn))
        return carry

    lax.fori_loop(1, 3 * quarter, send_far, 0)
    lax.fori_loop(1, quarter, send_near, 0)
    spread_out(values_out, values_in, 0)
    c_in[me] = pick_c(me)
    load_j.wait()
    load_w.wait()
    load_sample.wait()
    for load in load_b:
        load.wait()

    def pick_b(part, carry):
        picked = pick_columns(folded_b, j_ref[part] - me * b_rows, rank)
        b_weighted[part] = w_ref[part] * picked
        return carry

    lax.fori_loop(0, n, pick_b, 0)
    columns = lax.broadcasted_iota(jnp.int32, (blocks, chunk), 1)
    sample_column[...] = block_column(sample_ref)

    def add_chunk(part, carry):
        gram, picks = carry
        weights = w_ref[part]
        sketch = b_weighted[part] * c_in[part].astype(jnp.float32)
        top = sketch.astype(jnp.bfloat16)
        rest = (sketch - top.astype(jnp.float32)).astype(jnp.bfloat16)
        both = jnp.concatenate([top, rest], axis=0)
        gram = gram + lax.dot_general(both, both, NT, preferred_element_type=jnp.float32)
        weighted = (weights * sketch).astype(jnp.bfloat16)
        chosen = columns == sample_column[...] - part * chunk
        chosen = jnp.where(chosen, 1.0, 0.0).astype(jnp.bfloat16)
        picks = picks + lax.dot_general(
            chosen, weighted, NT, preferred_element_type=jnp.float32
        )
        return gram, picks

    def add_peer(part, carry):
        copy_c(part, part).wait_recv()
        return add_chunk(part, carry)

    carry = (
        jnp.zeros((2 * rank, 2 * rank), jnp.float32),
        jnp.zeros((blocks, rank), jnp.float32),
    )
    carry = add_chunk(me, carry)
    carry = lax.fori_loop(
        0, quarter, lambda turn, carry: add_peer(member(1 + 2 * inner, turn), carry), carry
    )
    carry = lax.fori_loop(
        1, quarter, lambda turn, carry: add_peer(sibling(turn), carry), carry
    )
    gram, picks = lax.fori_loop(
        0, 2 * quarter, lambda turn, carry: add_peer(late_turn(turn), carry), carry
    )

    pair = gram[:rank] + gram[rank:]
    pair = (pair + pltpu.roll(pair, rank, 1)) / total_samples
    pair_rows = lax.broadcasted_iota(jnp.int32, pair.shape, 0)
    pair_lanes = lax.broadcasted_iota(jnp.int32, pair.shape, 1)
    ridge = 0.05 * live_local / total_rows
    pair = pair + jnp.where(pair_lanes % rank == pair_rows, ridge, 0.0)
    scatter(pair, gram_out, gram_in, 1)
    rows_half = per_peer // 2
    picks = picks.reshape(n, per_peer, rank)
    picks_out[...] = jnp.concatenate(
        [picks[:, :rows_half], picks[:, rows_half:]], axis=2
    ).astype(jnp.bfloat16)
    picks_in[me] = picks_out[me]
    spread_out(picks_out, picks_in, 2)
    others(0, values_in).wait_recv()
    arrived = values_in[...].astype(jnp.float32)
    tile_of = lax.broadcasted_iota(jnp.int32, (n * rows_half, 128), 0) % rows_half // slots
    for part in range(2):
        rows = arrived[:, part * rows_half : (part + 1) * rows_half, :].reshape(-1, 128)
        spread_ref[part] = jnp.concatenate(
            [jnp.where(tile_of == tile, rows, 0.0) for tile in range(tiles // 2)], axis=1
        ).astype(jnp.bfloat16)

    others(1, gram_in).wait_recv()
    gather(gram_in, share_out, share_in, 3)
    others(2, picks_in).wait_recv()
    arrived = picks_in[...].astype(jnp.float32).reshape(-1, 2 * rank).astype(jnp.bfloat16)
    gathered = jnp.concatenate(
        [
            lax.dot_general(arrived, spread_ref[part], TN, preferred_element_type=jnp.float32)[
                part * rank : (part + 1) * rank
            ]
            for part in range(2)
        ],
        axis=1,
    )
    moment = lax.dot_general(
        gathered,
        jnp.concatenate([gathered, gathered], axis=0),
        NT,
        precision=lax.Precision.HIGHEST,
        preferred_element_type=jnp.float32,
    )
    scatter(moment, moment_out, moment_in, 4)
    others(3, share_in).wait_recv()
    others(4, moment_in).wait_recv()
    gather(moment_in, moments_out, moments_in, 5)
    total = whole(share_in)
    inverted = inverse(total)
    update = jnp.dot(
        inverted,
        gathered,
        precision=lax.Precision.HIGHEST,
        preferred_element_type=jnp.float32,
    )
    gram_rows = lax.broadcasted_iota(jnp.int32, (rank, rank), 0)
    diagonal = gram_rows == lax.broadcasted_iota(jnp.int32, (rank, rank), 1)
    others(5, moments_in).wait_recv()
    solved = jnp.dot(
        inverted,
        whole(moments_in),
        precision=lax.Precision.HIGHEST,
        preferred_element_type=jnp.float32,
    )
    squares = jnp.sum(solved * inverted, axis=1, keepdims=True)
    scales = jnp.sqrt(jnp.maximum(squares, 0.0) / total_rows + 1e-06)
    out_ref[...] = (update / scales).astype(out_ref.dtype)
    scales_ref[...] = jnp.sum(jnp.where(diagonal, scales, 0.0), axis=0, keepdims=True)

    each_peer(lambda peer: copy_c(peer, me).wait_send())
    others(0, values_out).wait_send()
    others(1, gram_out).wait_send()
    others(2, picks_out).wait_send()
    others(3, share_in).wait_send()
    others(4, moment_out).wait_send()
    others(5, moments_in).wait_send()


def shards(
    factor_b, factor_c, sample_j, sample_k, sample_weight, block_values, block_sample, block_count
):
    rank, b_rows = factor_b.shape
    n, _, chunk = sample_k.shape
    _, _, tiles, slots, tile_rows = block_values.shape
    samples = sample_j.shape[0]
    per_peer = tiles * slots
    blocks = n * per_peer
    width = 512
    piece = max(rank // (2 * n), 1)
    bf16, f32, i32 = jnp.bfloat16, jnp.float32, jnp.int32
    hbm = pl.BlockSpec(memory_space=pltpu.HBM)
    vmem = pl.BlockSpec(memory_space=pltpu.VMEM)
    factor_new, scales = pl.pallas_call(
        functools.partial(kernel, n, tiles, slots, tiles * tile_rows * n, samples * n),
        out_shape=(
            pltpu.VMEM((rank, tiles * tile_rows), bf16),
            pltpu.VMEM((1, rank), f32),
        ),
        in_specs=[hbm] * 8,
        out_specs=(vmem, vmem),
        scratch_shapes=[
            pltpu.VMEM((b_rows // width * rank, width), bf16),
            pltpu.VMEM((factor_c.shape[1] // width * rank, width), bf16),
            pltpu.VMEM((n, 1, chunk), i32),
            pltpu.VMEM((n, 1, chunk), i32),
            pltpu.VMEM((n, 1, chunk), f32),
            pltpu.VMEM((blocks, tile_rows), bf16),
            pltpu.VMEM((tiles, slots, n), i32),
            pltpu.VMEM((tiles, slots, n), i32),
            pltpu.VMEM((n, rank, chunk), bf16),
            pltpu.VMEM((n, rank, chunk), bf16),
            pltpu.VMEM((n, rank, chunk), f32),
            pltpu.VMEM((n, per_peer, tile_rows), bf16),
            pltpu.VMEM((n, per_peer, tile_rows), bf16),
            pltpu.VMEM((2, blocks // 2, tiles // 2 * tile_rows), bf16),
            pltpu.VMEM((n, per_peer // 2, 2 * rank), bf16),
            pltpu.VMEM((n, per_peer // 2, 2 * rank), bf16),
            pltpu.VMEM((n, piece, 2 * rank), f32),
            pltpu.VMEM((n, piece, 2 * rank), f32),
            pltpu.VMEM((piece, 2 * rank), f32),
            pltpu.VMEM((n, piece, 2 * rank), f32),
            pltpu.VMEM((blocks, 1), i32),
            pltpu.VMEM((n, piece, 2 * rank), f32),
            pltpu.VMEM((n, piece, 2 * rank), f32),
            pltpu.VMEM((piece, 2 * rank), f32),
            pltpu.VMEM((n, piece, 2 * rank), f32),
            pltpu.SemaphoreType.DMA((8,)),
            pltpu.SemaphoreType.DMA((n,)),
            pltpu.SemaphoreType.DMA((n,)),
            pltpu.SemaphoreType.DMA((6,)),
            pltpu.SemaphoreType.DMA((6,)),
        ],
        compiler_params=pltpu.CompilerParams(collective_id=0, has_side_effects=True),
    )(
        factor_b,
        factor_c,
        sample_j.reshape(n, 1, chunk),
        sample_k,
        sample_weight.reshape(n, 1, chunk),
        block_values.reshape(blocks, tile_rows),
        block_sample[0].transpose(1, 2, 0),
        block_count[0].transpose(1, 2, 0),
    )
    return factor_new, scales.reshape(rank)


def solution(mesh):
    in_specs = (
        P(None, ("groups", "row")),
        P(None, ("groups", "row")),
        P(("groups", "row")),
        P(None, ("groups", "row"), None),
        P(("groups", "row")),
        P(("groups", "row"), None, None, None, None),
        P(("groups", "row"), None, None, None),
        P(("groups", "row"), None, None, None),
    )
    out_specs = (P(None, ("groups", "row")), P("groups"))
    return jax.shard_map(shards, mesh=mesh, in_specs=in_specs, out_specs=out_specs, check_vma=False)
```

```python
import functools

import jax
import jax.numpy as jnp
from jax import lax
from jax.experimental import pallas as pl
from jax.experimental.pallas import tpu as pltpu
from jax.sharding import PartitionSpec as P

NT = (((1,), (1,)), ((), ()))
TN = (((0,), (0,)), ((), ()))
MESH = pl.DeviceIdType.MESH
UNROLLED_PEERS = 16
PANEL = 4


def pick_columns(folded, index, rank):
    width = folded.shape[1]
    count = index.shape[1]
    low = lax.rem(index, width)
    high = lax.div(index, width)
    rows = lax.broadcasted_iota(jnp.int16, (width, count), 0)
    one_hot = jnp.where(rows == low.astype(jnp.int16), jnp.bfloat16(1), jnp.bfloat16(0))
    products = jnp.dot(folded[...], one_hot, preferred_element_type=jnp.float32)
    picked = products[:rank]
    high = jnp.broadcast_to(high, (rank, count))
    for part in range(1, folded.shape[0] // rank):
        picked = jnp.where(high == part, products[part * rank : (part + 1) * rank], picked)
    return picked


def block_column(table_ref):
    table = jnp.concatenate([table_ref[tile] for tile in range(table_ref.shape[0])], axis=0)
    return jnp.concatenate(
        [table[:, peer : peer + 1] for peer in range(table.shape[1])], axis=0
    )


def inverse(matrix):
    order = matrix.shape[0]
    lanes = lax.broadcasted_iota(jnp.int32, (1, order), 1)
    rows = lax.broadcasted_iota(jnp.int32, (order, 1), 0)
    for first in range(0, order, PANEL):
        panel = [
            jnp.broadcast_to(matrix[:, k : k + 1], matrix.shape)
            for k in range(first, first + PANEL)
        ]
        for step in range(PANEL):
            k = first + step
            column = panel[step]
            pivot = 1.0 / column[k : k + 1, :]
            scaled = jnp.where(lanes == k, 1.0, matrix[k : k + 1, :]) * pivot
            own = rows == k
            matrix = jnp.where(
                own, scaled, jnp.where(lanes == k, 0.0, matrix) - column * scaled
            )
            for later in range(step + 1, PANEL):
                factor = panel[later][k : k + 1, :] * pivot
                panel[later] = jnp.where(own, factor, panel[later] - column * factor)
    return matrix


def kernel(
    n,
    tiles,
    slots,
    total_rows,
    total_samples,
    b_hbm,
    c_hbm,
    j_hbm,
    k_hbm,
    w_hbm,
    values_hbm,
    sample_hbm,
    count_hbm,
    out_ref,
    scales_ref,
    folded_b,
    folded_c,
    j_ref,
    k_ref,
    w_ref,
    values_ref,
    sample_ref,
    count_ref,
    c_out,
    c_in,
    b_weighted,
    values_out,
    values_in,
    spread_ref,
    picks_out,
    picks_in,
    gram_out,
    gram_in,
    share_out,
    share_in,
    sample_column,
    moment_out,
    moment_in,
    moments_out,
    moments_in,
    load_sems,
    c_send,
    c_recv,
    send_sems,
    recv_sems,
    turn_sem,
):
    me = lax.axis_index("row")
    rank, b_rows = b_hbm.shape
    c_rows = c_hbm.shape[1]
    width = folded_c.shape[1]
    per_peer = tiles * slots
    blocks = n * per_peer
    chunk = c_in.shape[2]
    quarter = n // 4
    own = me // quarter
    place = me % quarter
    side = own // 2
    inner = (own + side) % 2

    def member(frame, turn):
        return (frame + side * (3 - 2 * frame)) * quarter + (place + turn) % quarter

    def sibling(turn):
        return own * quarter + (place + turn) % quarter

    def send_turn(turn):
        block = turn // quarter
        first, last = (2 - block) // 2, block // 2
        frame = first * (2 - 2 * inner) + (1 - first - last) * 3 + last * (1 + inner)
        return member(frame, turn % quarter)

    def late_turn(turn):
        block = turn // quarter
        return member((1 - block) * (3 - 3 * inner) + block * 2, quarter - turn % quarter)

    def loop(start, stop, body):
        if n <= UNROLLED_PEERS:
            for turn in range(start, stop):
                body(turn)
        else:
            lax.fori_loop(start, stop, lambda turn, carry: (body(turn), carry)[1], 0)

    def each_peer(body):
        for frame in (3, 2, 1 - inner):
            loop(0, quarter, lambda turn, frame=frame: body(member(frame, turn)))
        loop(1, quarter, lambda turn: body(sibling(turn)))

    def remote(peer, source, target, send, recv):
        return pltpu.make_async_remote_copy(
            src_ref=source,
            dst_ref=target,
            send_sem=send,
            recv_sem=recv,
            device_id={"row": peer},
            device_id_type=MESH,
        )

    def copy_c(peer, slot):
        return remote(peer, c_out.at[peer], c_in.at[slot], c_send.at[peer], c_recv.at[slot])

    def others(kind, target):
        region = target.at[pl.ds(0, n - 1)]
        return remote(sibling(1), region, region, send_sems.at[kind], recv_sems.at[kind])

    def spread_out(source, target, kind):
        each_peer(
            lambda peer: remote(
                peer, source.at[peer], target.at[me], send_sems.at[kind], recv_sems.at[kind]
            ).start()
        )

    piece = gram_out.shape[1]
    fold = rank // (n * piece)

    def scatter(pair, source, target, kind):
        if fold == 2:
            upper = lax.broadcasted_iota(jnp.int32, (rank // 2, 2 * rank), 1) < rank
            pair = jnp.where(upper, pair[: rank // 2], pair[rank // 2 :])
        for part in range(n):
            source[part] = pair[part * piece : (part + 1) * piece]
        target[me] = source[me]
        spread_out(source, target, kind)

    def gather(arrived, source, target, kind):
        source[...] = jnp.sum(arrived[...], axis=0)
        target[me] = source[...]
        each_peer(
            lambda peer: remote(
                peer, source, target.at[me], send_sems.at[kind], recv_sems.at[kind]
            ).start()
        )

    def whole(arrived):
        matrix = jnp.concatenate([arrived[part] for part in range(n)], axis=0)
        if fold == 2:
            return jnp.concatenate([matrix[:, :rank], matrix[:, rank:]], axis=0)
        return matrix[:, :rank]

    barrier = pltpu.get_barrier_semaphore()
    each_peer(
        lambda peer: pl.semaphore_signal(
            barrier, inc=1, device_id={"row": peer}, device_id_type=MESH
        )
    )

    def load_table(source, target, kind):
        return [
            pltpu.make_async_copy(
                source.at[:, pl.ds(part * width, width)],
                target.at[pl.ds(part * rank, rank)],
                load_sems.at[kind],
            )
            for part in range(source.shape[1] // width)
        ]

    load_c = load_table(c_hbm, folded_c, 0)
    load_b = load_table(b_hbm, folded_b, 1)
    load_k = pltpu.make_async_copy(k_hbm, k_ref, load_sems.at[2])
    load_j = pltpu.make_async_copy(j_hbm, j_ref, load_sems.at[3])
    load_w = pltpu.make_async_copy(w_hbm, w_ref, load_sems.at[4])
    load_values = pltpu.make_async_copy(values_hbm, values_ref, load_sems.at[5])
    load_sample = pltpu.make_async_copy(sample_hbm, sample_ref, load_sems.at[6])
    load_count = pltpu.make_async_copy(count_hbm, count_ref, load_sems.at[7])
    for load in [load_k, *load_c, load_count, load_values, load_sample, load_j, *load_b, load_w]:
        load.start()

    def pick_c(peer):
        return pick_columns(folded_c, k_ref[peer] - me * c_rows, rank).astype(jnp.bfloat16)

    load_k.wait()
    for load in load_c:
        load.wait()
    c_out[send_turn(0)] = pick_c(send_turn(0))
    load_count.wait()
    load_values.wait()
    lanes = lax.broadcasted_iota(jnp.int32, (blocks, 128), 1)
    counts = block_column(count_ref)
    live = lanes < counts
    masked = jnp.where(live, values_ref[...].astype(jnp.float32), 0.0).astype(jnp.bfloat16)
    values_out[...] = masked.reshape(values_out.shape)
    values_in[me] = values_out[me]
    live_local = jnp.sum(counts.astype(jnp.float32), axis=0, keepdims=True)
    pl.semaphore_wait(barrier, n - 1)
    copy_c(send_turn(0), me).start()

    def send_c(peer):
        c_out[peer] = pick_c(peer)
        copy_c(peer, me).start()

    def send_far(turn, carry):
        send_c(send_turn(turn))
        return carry

    def send_near(turn, carry):
        send_c(sibling(turn))
        return carry

    lax.fori_loop(1, 3 * quarter, send_far, 0)
    lax.fori_loop(1, quarter, send_near, 0)

    @pl.when(inner == 1)
    def _():
        spread_out(values_out, values_in, 0)

    c_in[me] = pick_c(me)
    load_j.wait()
    load_w.wait()
    load_sample.wait()
    for load in load_b:
        load.wait()

    def pick_b(part, carry):
        picked = pick_columns(folded_b, j_ref[part] - me * b_rows, rank)
        b_weighted[part] = w_ref[part] * picked
        return carry

    lax.fori_loop(0, n, pick_b, 0)
    columns = lax.broadcasted_iota(jnp.int32, (blocks, chunk), 1)
    sample_column[...] = block_column(sample_ref)

    def add_chunk(part, carry):
        gram, picks = carry
        weights = w_ref[part]
        sketch = b_weighted[part] * c_in[part].astype(jnp.float32)
        top = sketch.astype(jnp.bfloat16)
        rest = (sketch - top.astype(jnp.float32)).astype(jnp.bfloat16)
        both = jnp.concatenate([top, rest], axis=0)
        gram = gram + lax.dot_general(both, both, NT, preferred_element_type=jnp.float32)
        weighted = (weights * sketch).astype(jnp.bfloat16)
        chosen = columns == sample_column[...] - part * chunk
        chosen = jnp.where(chosen, 1.0, 0.0).astype(jnp.bfloat16)
        picks = picks + lax.dot_general(
            chosen, weighted, NT, preferred_element_type=jnp.float32
        )
        return gram, picks

    def add_peer(part, carry):
        copy_c(part, part).wait_recv()
        return add_chunk(part, carry)

    carry = (
        jnp.zeros((2 * rank, 2 * rank), jnp.float32),
        jnp.zeros((blocks, rank), jnp.float32),
    )
    carry = add_chunk(me, carry)
    carry = lax.fori_loop(
        0, quarter, lambda turn, carry: add_peer(member(1 + 2 * inner, quarter - turn), carry), carry
    )
    carry = lax.fori_loop(
        1, quarter, lambda turn, carry: add_peer(sibling(quarter - turn), carry), carry
    )

    def add_late(turn, carry):
        carry = add_peer(late_turn(turn), carry)

        @pl.when((inner == 1) & (turn == 3 * quarter // 2 - 1))
        def _():
            pl.semaphore_signal(
                turn_sem, inc=1, device_id={"row": member(0, 0)}, device_id_type=MESH
            )

        return carry

    gram, picks = lax.fori_loop(0, 2 * quarter, add_late, carry)

    @pl.when(inner == 0)
    def _():
        pl.semaphore_wait(turn_sem, 1)
        spread_out(values_out, values_in, 0)

    rows_half = per_peer // 2
    picks = picks.reshape(n, per_peer, rank)
    picks_out[...] = jnp.concatenate(
        [picks[:, :rows_half], picks[:, rows_half:]], axis=2
    ).astype(jnp.bfloat16)
    picks_in[me] = picks_out[me]
    spread_out(picks_out, picks_in, 2)

    pair = gram[:rank] + gram[rank:]
    pair = (pair + pltpu.roll(pair, rank, 1)) / total_samples
    pair_rows = lax.broadcasted_iota(jnp.int32, pair.shape, 0)
    pair_lanes = lax.broadcasted_iota(jnp.int32, pair.shape, 1)
    ridge = 0.05 * live_local / total_rows
    pair = pair + jnp.where(pair_lanes % rank == pair_rows, ridge, 0.0)
    scatter(pair, gram_out, gram_in, 1)

    others(0, values_in).wait_recv()
    arrived = values_in[...].astype(jnp.float32)
    tile_of = lax.broadcasted_iota(jnp.int32, (n * rows_half, 128), 0) % rows_half // slots
    for part in range(2):
        rows = arrived[:, part * rows_half : (part + 1) * rows_half, :].reshape(-1, 128)
        spread_ref[part] = jnp.concatenate(
            [jnp.where(tile_of == tile, rows, 0.0) for tile in range(tiles // 2)], axis=1
        ).astype(jnp.bfloat16)

    others(2, picks_in).wait_recv()
    arrived = picks_in[...].astype(jnp.float32).reshape(-1, 2 * rank).astype(jnp.bfloat16)
    gathered = jnp.concatenate(
        [
            lax.dot_general(arrived, spread_ref[part], TN, preferred_element_type=jnp.float32)[
                part * rank : (part + 1) * rank
            ]
            for part in range(2)
        ],
        axis=1,
    )
    moment = lax.dot_general(
        gathered,
        jnp.concatenate([gathered, gathered], axis=0),
        NT,
        precision=lax.Precision.HIGHEST,
        preferred_element_type=jnp.float32,
    )
    scatter(moment, moment_out, moment_in, 4)
    others(1, gram_in).wait_recv()
    gather(gram_in, share_out, share_in, 3)
    others(4, moment_in).wait_recv()
    gather(moment_in, moments_out, moments_in, 5)
    others(3, share_in).wait_recv()
    total = whole(share_in)
    inverted = inverse(total)
    update = jnp.dot(
        inverted,
        gathered,
        precision=lax.Precision.HIGHEST,
        preferred_element_type=jnp.float32,
    )
    gram_rows = lax.broadcasted_iota(jnp.int32, (rank, rank), 0)
    diagonal = gram_rows == lax.broadcasted_iota(jnp.int32, (rank, rank), 1)
    others(5, moments_in).wait_recv()
    solved = jnp.dot(
        inverted,
        whole(moments_in),
        precision=lax.Precision.HIGHEST,
        preferred_element_type=jnp.float32,
    )
    squares = jnp.sum(solved * inverted, axis=1, keepdims=True)
    scales = jnp.sqrt(jnp.maximum(squares, 0.0) / total_rows + 1e-06)
    out_ref[...] = (update / scales).astype(out_ref.dtype)
    scales_ref[...] = jnp.sum(jnp.where(diagonal, scales, 0.0), axis=0, keepdims=True)

    each_peer(lambda peer: copy_c(peer, me).wait_send())
    others(0, values_out).wait_send()
    others(1, gram_out).wait_send()
    others(2, picks_out).wait_send()
    others(3, share_in).wait_send()
    others(4, moment_out).wait_send()
    others(5, moments_in).wait_send()


def shards(
    factor_b, factor_c, sample_j, sample_k, sample_weight, block_values, block_sample, block_count
):
    rank, b_rows = factor_b.shape
    n, _, chunk = sample_k.shape
    _, _, tiles, slots, tile_rows = block_values.shape
    samples = sample_j.shape[0]
    per_peer = tiles * slots
    blocks = n * per_peer
    width = 512
    piece = max(rank // (2 * n), 1)
    bf16, f32, i32 = jnp.bfloat16, jnp.float32, jnp.int32
    hbm = pl.BlockSpec(memory_space=pltpu.HBM)
    vmem = pl.BlockSpec(memory_space=pltpu.VMEM)
    factor_new, scales = pl.pallas_call(
        functools.partial(kernel, n, tiles, slots, tiles * tile_rows * n, samples * n),
        out_shape=(
            pltpu.VMEM((rank, tiles * tile_rows), bf16),
            pltpu.VMEM((1, rank), f32),
        ),
        in_specs=[hbm] * 8,
        out_specs=(vmem, vmem),
        scratch_shapes=[
            pltpu.VMEM((b_rows // width * rank, width), bf16),
            pltpu.VMEM((factor_c.shape[1] // width * rank, width), bf16),
            pltpu.VMEM((n, 1, chunk), i32),
            pltpu.VMEM((n, 1, chunk), i32),
            pltpu.VMEM((n, 1, chunk), f32),
            pltpu.VMEM((blocks, tile_rows), bf16),
            pltpu.VMEM((tiles, slots, n), i32),
            pltpu.VMEM((tiles, slots, n), i32),
            pltpu.VMEM((n, rank, chunk), bf16),
            pltpu.VMEM((n, rank, chunk), bf16),
            pltpu.VMEM((n, rank, chunk), f32),
            pltpu.VMEM((n, per_peer, tile_rows), bf16),
            pltpu.VMEM((n, per_peer, tile_rows), bf16),
            pltpu.VMEM((2, blocks // 2, tiles // 2 * tile_rows), bf16),
            pltpu.VMEM((n, per_peer // 2, 2 * rank), bf16),
            pltpu.VMEM((n, per_peer // 2, 2 * rank), bf16),
            pltpu.VMEM((n, piece, 2 * rank), f32),
            pltpu.VMEM((n, piece, 2 * rank), f32),
            pltpu.VMEM((piece, 2 * rank), f32),
            pltpu.VMEM((n, piece, 2 * rank), f32),
            pltpu.VMEM((blocks, 1), i32),
            pltpu.VMEM((n, piece, 2 * rank), f32),
            pltpu.VMEM((n, piece, 2 * rank), f32),
            pltpu.VMEM((piece, 2 * rank), f32),
            pltpu.VMEM((n, piece, 2 * rank), f32),
            pltpu.SemaphoreType.DMA((8,)),
            pltpu.SemaphoreType.DMA((n,)),
            pltpu.SemaphoreType.DMA((n,)),
            pltpu.SemaphoreType.DMA((6,)),
            pltpu.SemaphoreType.DMA((6,)),
            pltpu.SemaphoreType.REGULAR,
        ],
        compiler_params=pltpu.CompilerParams(collective_id=0, has_side_effects=True),
    )(
        factor_b,
        factor_c,
        sample_j.reshape(n, 1, chunk),
        sample_k,
        sample_weight.reshape(n, 1, chunk),
        block_values.reshape(blocks, tile_rows),
        block_sample[0].transpose(1, 2, 0),
        block_count[0].transpose(1, 2, 0),
    )
    return factor_new, scales.reshape(rank)


def solution(mesh):
    in_specs = (
        P(None, ("groups", "row")),
        P(None, ("groups", "row")),
        P(("groups", "row")),
        P(None, ("groups", "row"), None),
        P(("groups", "row")),
        P(("groups", "row"), None, None, None, None),
        P(("groups", "row"), None, None, None),
        P(("groups", "row"), None, None, None),
    )
    out_specs = (P(None, ("groups", "row")), P("groups"))
    return jax.shard_map(shards, mesh=mesh, in_specs=in_specs, out_specs=out_specs, check_vma=False)
```

```python
import functools

import jax
import jax.numpy as jnp
from jax import lax
from jax.experimental import pallas as pl
from jax.experimental.pallas import tpu as pltpu
from jax.sharding import PartitionSpec as P

NN = (((1,), (0,)), ((), ()))
NT = (((1,), (1,)), ((), ()))
TN = (((0,), (0,)), ((), ()))
MESH = pl.DeviceIdType.MESH
UNROLLED_PEERS = 16
PANEL = 4


def pick_columns(folded, index, rank):
    width = folded.shape[1]
    count = index.shape[1]
    low = lax.rem(index, width)
    high = lax.div(index, width)
    rows = lax.broadcasted_iota(jnp.int16, (width, count), 0)
    one_hot = jnp.where(rows == low.astype(jnp.int16), jnp.bfloat16(1), jnp.bfloat16(0))
    products = jnp.dot(folded[...], one_hot, preferred_element_type=jnp.float32)
    picked = products[:rank]
    high = jnp.broadcast_to(high, (rank, count))
    for part in range(1, folded.shape[0] // rank):
        picked = jnp.where(high == part, products[part * rank : (part + 1) * rank], picked)
    return picked


def block_column(table_ref):
    table = jnp.concatenate([table_ref[tile] for tile in range(table_ref.shape[0])], axis=0)
    return jnp.concatenate(
        [table[:, peer : peer + 1] for peer in range(table.shape[1])], axis=0
    )


def product(left, right, dimensions=NT):
    return lax.dot_general(
        left,
        right,
        dimensions,
        precision=lax.Precision.HIGHEST,
        preferred_element_type=jnp.float32,
    )


def inverse(matrix):
    order = matrix.shape[0]
    lanes = lax.broadcasted_iota(jnp.int32, (1, order), 1)
    rows = lax.broadcasted_iota(jnp.int32, (order, 1), 0)
    for first in range(0, order, PANEL):
        panel = [
            jnp.broadcast_to(matrix[:, k : k + 1], matrix.shape)
            for k in range(first, first + PANEL)
        ]
        for step in range(PANEL):
            k = first + step
            column = panel[step]
            pivot = 1.0 / column[k : k + 1, :]
            scaled = jnp.where(lanes == k, 1.0, matrix[k : k + 1, :]) * pivot
            own = rows == k
            matrix = jnp.where(
                own, scaled, jnp.where(lanes == k, 0.0, matrix) - column * scaled
            )
            for later in range(step + 1, PANEL):
                factor = panel[later][k : k + 1, :] * pivot
                panel[later] = jnp.where(own, factor, panel[later] - column * factor)
    return matrix


def kernel(
    n,
    tiles,
    slots,
    total_rows,
    total_samples,
    b_hbm,
    c_hbm,
    j_hbm,
    k_hbm,
    w_hbm,
    values_hbm,
    sample_hbm,
    count_hbm,
    out_ref,
    scales_ref,
    folded_b,
    folded_c,
    j_ref,
    k_ref,
    w_ref,
    values_ref,
    sample_ref,
    count_ref,
    c_out,
    c_in,
    b_weighted,
    values_out,
    values_in,
    spread_ref,
    picks_out,
    picks_in,
    gram_out,
    gram_in,
    share_out,
    share_in,
    sample_column,
    moment_out,
    moment_in,
    load_sems,
    c_send,
    c_recv,
    send_sems,
    recv_sems,
    turn_sem,
):
    me = lax.axis_index("row")
    rank, b_rows = b_hbm.shape
    c_rows = c_hbm.shape[1]
    width = folded_c.shape[1]
    per_peer = tiles * slots
    blocks = n * per_peer
    chunk = c_in.shape[2]
    quarter = n // 4
    own = me // quarter
    place = me % quarter
    side = own // 2
    inner = (own + side) % 2

    def member(frame, turn):
        return (frame + side * (3 - 2 * frame)) * quarter + (place + turn) % quarter

    def sibling(turn):
        return own * quarter + (place + turn) % quarter

    def send_turn(turn):
        block = turn // quarter
        first, last = (2 - block) // 2, block // 2
        frame = first * (2 - 2 * inner) + (1 - first - last) * 3 + last * (1 + inner)
        return member(frame, turn % quarter)

    def late_turn(turn):
        block = turn // quarter
        return member((1 - block) * (3 - 3 * inner) + block * 2, quarter - turn % quarter)

    def loop(start, stop, body):
        if n <= UNROLLED_PEERS:
            for turn in range(start, stop):
                body(turn)
        else:
            lax.fori_loop(start, stop, lambda turn, carry: (body(turn), carry)[1], 0)

    def each_peer(body):
        for frame in (3, 2, 1 - inner):
            loop(0, quarter, lambda turn, frame=frame: body(member(frame, turn)))
        loop(1, quarter, lambda turn: body(sibling(turn)))

    def remote(peer, source, target, send, recv):
        return pltpu.make_async_remote_copy(
            src_ref=source,
            dst_ref=target,
            send_sem=send,
            recv_sem=recv,
            device_id={"row": peer},
            device_id_type=MESH,
        )

    def copy_c(peer, slot):
        return remote(peer, c_out.at[peer], c_in.at[slot], c_send.at[peer], c_recv.at[slot])

    def others(kind, target):
        region = target.at[pl.ds(0, n - 1)]
        return remote(sibling(1), region, region, send_sems.at[kind], recv_sems.at[kind])

    def spread_out(source, target, kind):
        each_peer(
            lambda peer: remote(
                peer, source.at[peer], target.at[me], send_sems.at[kind], recv_sems.at[kind]
            ).start()
        )

    def broadcast(source, target, kind):
        each_peer(
            lambda peer: remote(
                peer, source, target.at[me], send_sems.at[kind], recv_sems.at[kind]
            ).start()
        )

    piece = gram_out.shape[1]
    fold = rank // (n * piece)

    def scatter(pair, source, target, kind):
        if fold == 2:
            upper = lax.broadcasted_iota(jnp.int32, (rank // 2, 2 * rank), 1) < rank
            pair = jnp.where(upper, pair[: rank // 2], pair[rank // 2 :])
        for part in range(n):
            source[part] = pair[part * piece : (part + 1) * piece]
        target[me] = source[me]
        spread_out(source, target, kind)

    def gather(arrived, source, target, kind):
        source[...] = jnp.sum(arrived[...], axis=0)
        target[me] = source[...]
        broadcast(source, target, kind)

    def whole(arrived):
        matrix = jnp.concatenate([arrived[part] for part in range(n)], axis=0)
        if fold == 2:
            return jnp.concatenate([matrix[:, :rank], matrix[:, rank:]], axis=0)
        return matrix[:, :rank]

    barrier = pltpu.get_barrier_semaphore()
    each_peer(
        lambda peer: pl.semaphore_signal(
            barrier, inc=1, device_id={"row": peer}, device_id_type=MESH
        )
    )

    def load_table(source, target, kind):
        return [
            pltpu.make_async_copy(
                source.at[:, pl.ds(part * width, width)],
                target.at[pl.ds(part * rank, rank)],
                load_sems.at[kind],
            )
            for part in range(source.shape[1] // width)
        ]

    load_c = load_table(c_hbm, folded_c, 0)
    load_b = load_table(b_hbm, folded_b, 1)
    load_k = pltpu.make_async_copy(k_hbm, k_ref, load_sems.at[2])
    load_j = pltpu.make_async_copy(j_hbm, j_ref, load_sems.at[3])
    load_w = pltpu.make_async_copy(w_hbm, w_ref, load_sems.at[4])
    load_values = pltpu.make_async_copy(values_hbm, values_ref, load_sems.at[5])
    load_sample = pltpu.make_async_copy(sample_hbm, sample_ref, load_sems.at[6])
    load_count = pltpu.make_async_copy(count_hbm, count_ref, load_sems.at[7])
    for load in [load_k, *load_c, load_count, load_values, load_sample, load_j, *load_b, load_w]:
        load.start()

    def pick_c(peer):
        return pick_columns(folded_c, k_ref[peer] - me * c_rows, rank).astype(jnp.bfloat16)

    load_k.wait()
    for load in load_c:
        load.wait()
    c_out[send_turn(0)] = pick_c(send_turn(0))
    load_count.wait()
    load_values.wait()
    lanes = lax.broadcasted_iota(jnp.int32, (blocks, 128), 1)
    counts = block_column(count_ref)
    live = lanes < counts
    masked = jnp.where(live, values_ref[...].astype(jnp.float32), 0.0).astype(jnp.bfloat16)
    values_out[...] = masked.reshape(values_out.shape)
    values_in[me] = values_out[me]
    live_local = jnp.sum(counts.astype(jnp.float32), axis=0, keepdims=True)
    pl.semaphore_wait(barrier, n - 1)
    copy_c(send_turn(0), me).start()

    def send_c(peer):
        c_out[peer] = pick_c(peer)
        copy_c(peer, me).start()

    def send_far(turn, carry):
        send_c(send_turn(turn))
        return carry

    def send_near(turn, carry):
        send_c(sibling(turn))
        return carry

    lax.fori_loop(1, 3 * quarter, send_far, 0)
    lax.fori_loop(1, quarter, send_near, 0)

    @pl.when(inner == 1)
    def _():
        spread_out(values_out, values_in, 0)

    c_in[me] = pick_c(me)
    load_j.wait()
    load_w.wait()
    load_sample.wait()
    for load in load_b:
        load.wait()

    def pick_b(part, carry):
        picked = pick_columns(folded_b, j_ref[part] - me * b_rows, rank)
        b_weighted[part] = w_ref[part] * picked
        return carry

    lax.fori_loop(0, n, pick_b, 0)
    columns = lax.broadcasted_iota(jnp.int32, (blocks, chunk), 1)
    sample_column[...] = block_column(sample_ref)

    def add_chunk(part, carry):
        gram, picks = carry
        weights = w_ref[part]
        sketch = b_weighted[part] * c_in[part].astype(jnp.float32)
        top = sketch.astype(jnp.bfloat16)
        rest = (sketch - top.astype(jnp.float32)).astype(jnp.bfloat16)
        both = jnp.concatenate([top, rest], axis=0)
        gram = gram + lax.dot_general(both, both, NT, preferred_element_type=jnp.float32)
        weighted = (weights * sketch).astype(jnp.bfloat16)
        chosen = columns == sample_column[...] - part * chunk
        chosen = jnp.where(chosen, 1.0, 0.0).astype(jnp.bfloat16)
        picks = picks + lax.dot_general(
            chosen, weighted, NT, preferred_element_type=jnp.float32
        )
        return gram, picks

    def add_peer(part, carry):
        copy_c(part, part).wait_recv()
        return add_chunk(part, carry)

    carry = (
        jnp.zeros((2 * rank, 2 * rank), jnp.float32),
        jnp.zeros((blocks, rank), jnp.float32),
    )
    carry = add_chunk(me, carry)
    carry = lax.fori_loop(
        0, quarter, lambda turn, carry: add_peer(member(1 + 2 * inner, quarter - turn), carry), carry
    )
    carry = lax.fori_loop(
        1, quarter, lambda turn, carry: add_peer(sibling(quarter - turn), carry), carry
    )

    def add_late(turn, carry):
        carry = add_peer(late_turn(turn), carry)

        @pl.when((inner == 1) & (turn == 3 * quarter // 2 - 1))
        def _():
            pl.semaphore_signal(
                turn_sem, inc=1, device_id={"row": member(0, 0)}, device_id_type=MESH
            )

        return carry

    gram, picks = lax.fori_loop(0, 2 * quarter, add_late, carry)

    @pl.when(inner == 0)
    def _():
        pl.semaphore_wait(turn_sem, 1)
        spread_out(values_out, values_in, 0)

    rows_half = per_peer // 2
    picks = picks.reshape(n, per_peer, rank)
    picks_out[...] = jnp.concatenate(
        [picks[:, :rows_half], picks[:, rows_half:]], axis=2
    ).astype(jnp.bfloat16)
    picks_in[me] = picks_out[me]
    spread_out(picks_out, picks_in, 2)

    pair = gram[:rank] + gram[rank:]
    pair = (pair + pltpu.roll(pair, rank, 1)) / total_samples
    pair_rows = lax.broadcasted_iota(jnp.int32, pair.shape, 0)
    pair_lanes = lax.broadcasted_iota(jnp.int32, pair.shape, 1)
    ridge = 0.05 * live_local / total_rows
    pair = pair + jnp.where(pair_lanes % rank == pair_rows, ridge, 0.0)
    scatter(pair, gram_out, gram_in, 1)

    others(0, values_in).wait_recv()
    arrived = values_in[...].astype(jnp.float32)
    tile_of = lax.broadcasted_iota(jnp.int32, (n * rows_half, 128), 0) % rows_half // slots
    for part in range(2):
        rows = arrived[:, part * rows_half : (part + 1) * rows_half, :].reshape(-1, 128)
        spread_ref[part] = jnp.concatenate(
            [jnp.where(tile_of == tile, rows, 0.0) for tile in range(tiles // 2)], axis=1
        ).astype(jnp.bfloat16)

    others(2, picks_in).wait_recv()
    arrived = picks_in[...].astype(jnp.float32).reshape(-1, 2 * rank).astype(jnp.bfloat16)
    gathered = jnp.concatenate(
        [
            lax.dot_general(arrived, spread_ref[part], TN, preferred_element_type=jnp.float32)[
                part * rank : (part + 1) * rank
            ]
            for part in range(2)
        ],
        axis=1,
    )
    others(1, gram_in).wait_recv()
    gather(gram_in, share_out, share_in, 3)

    part = rank // 2
    top = product(gathered[:part], jnp.concatenate([gathered] * 2, axis=0))
    low = product(gathered[part:], jnp.concatenate([gathered[part:]] * 4, axis=0))
    rows = lax.broadcasted_iota(jnp.int32, (part, 2 * rank), 0)
    lanes = lax.broadcasted_iota(jnp.int32, (part, 2 * rank), 1)
    across = lanes % rank
    triangle = jnp.where(across >= rows, jnp.where(across == rows, top, 2.0 * top), 2.0 * low)
    quarter_rows = part // 2
    moment_out[:quarter_rows] = jnp.where(
        lanes[:quarter_rows] < rank, triangle[:quarter_rows], triangle[quarter_rows:]
    )
    moment_out[quarter_rows:] = jnp.sum(
        jnp.where(lanes == rows, low, 0.0), axis=0, keepdims=True
    )
    moment_in[me] = moment_out[...]
    broadcast(moment_out, moment_in, 4)

    others(3, share_in).wait_recv()
    inverted = inverse(whole(share_in))
    update = product(inverted, gathered, NN)
    first = jnp.concatenate([inverted] * 2, axis=1)
    second = jnp.concatenate([inverted[:, part:]] * 4, axis=1)
    others(4, moment_in).wait_recv()
    moment = jnp.sum(moment_in[...], axis=0)
    triangle, corner = moment[:quarter_rows], moment[quarter_rows:]
    above = across >= rows
    stacked = jnp.concatenate([triangle] * 2, axis=0)
    stacked = jnp.where((lanes < rank) == (rows < quarter_rows), stacked, 0.0)
    zeros = jnp.zeros_like(stacked)
    stacked = jnp.concatenate(
        [
            jnp.concatenate([jnp.where(above, stacked, 0.0), zeros], axis=1),
            jnp.concatenate([zeros, jnp.where(above, 0.0, stacked)], axis=1),
        ],
        axis=0,
    )
    solved = product(inverted, stacked, NN)
    squares = jnp.sum(
        solved[:, : 2 * rank] * first
        + solved[:, 2 * rank :] * second
        + corner * second * second,
        axis=1,
        keepdims=True,
    )
    scales = jnp.sqrt(jnp.maximum(squares, 0.0) / total_rows + 1e-06)
    out_ref[...] = (update / scales).astype(out_ref.dtype)
    diagonal = lax.broadcasted_iota(jnp.int32, (rank, rank), 0)
    diagonal = diagonal == lax.broadcasted_iota(jnp.int32, (rank, rank), 1)
    scales_ref[...] = jnp.sum(jnp.where(diagonal, scales, 0.0), axis=0, keepdims=True)

    each_peer(lambda peer: copy_c(peer, me).wait_send())
    others(0, values_out).wait_send()
    others(1, gram_out).wait_send()
    others(2, picks_out).wait_send()
    others(3, share_in).wait_send()
    others(4, moment_in).wait_send()


def shards(
    factor_b, factor_c, sample_j, sample_k, sample_weight, block_values, block_sample, block_count
):
    rank, b_rows = factor_b.shape
    n, _, chunk = sample_k.shape
    _, _, tiles, slots, tile_rows = block_values.shape
    samples = sample_j.shape[0]
    per_peer = tiles * slots
    blocks = n * per_peer
    width = 512
    piece = max(rank // (2 * n), 1)
    bf16, f32, i32 = jnp.bfloat16, jnp.float32, jnp.int32
    hbm = pl.BlockSpec(memory_space=pltpu.HBM)
    vmem = pl.BlockSpec(memory_space=pltpu.VMEM)
    factor_new, scales = pl.pallas_call(
        functools.partial(kernel, n, tiles, slots, tiles * tile_rows * n, samples * n),
        out_shape=(
            pltpu.VMEM((rank, tiles * tile_rows), bf16),
            pltpu.VMEM((1, rank), f32),
        ),
        in_specs=[hbm] * 8,
        out_specs=(vmem, vmem),
        scratch_shapes=[
            pltpu.VMEM((b_rows // width * rank, width), bf16),
            pltpu.VMEM((factor_c.shape[1] // width * rank, width), bf16),
            pltpu.VMEM((n, 1, chunk), i32),
            pltpu.VMEM((n, 1, chunk), i32),
            pltpu.VMEM((n, 1, chunk), f32),
            pltpu.VMEM((blocks, tile_rows), bf16),
            pltpu.VMEM((tiles, slots, n), i32),
            pltpu.VMEM((tiles, slots, n), i32),
            pltpu.VMEM((n, rank, chunk), bf16),
            pltpu.VMEM((n, rank, chunk), bf16),
            pltpu.VMEM((n, rank, chunk), f32),
            pltpu.VMEM((n, per_peer, tile_rows), bf16),
            pltpu.VMEM((n, per_peer, tile_rows), bf16),
            pltpu.VMEM((2, blocks // 2, tiles // 2 * tile_rows), bf16),
            pltpu.VMEM((n, per_peer // 2, 2 * rank), bf16),
            pltpu.VMEM((n, per_peer // 2, 2 * rank), bf16),
            pltpu.VMEM((n, piece, 2 * rank), f32),
            pltpu.VMEM((n, piece, 2 * rank), f32),
            pltpu.VMEM((piece, 2 * rank), f32),
            pltpu.VMEM((n, piece, 2 * rank), f32),
            pltpu.VMEM((blocks, 1), i32),
            pltpu.VMEM((rank // 4 + 1, 2 * rank), f32),
            pltpu.VMEM((n, rank // 4 + 1, 2 * rank), f32),
            pltpu.SemaphoreType.DMA((8,)),
            pltpu.SemaphoreType.DMA((n,)),
            pltpu.SemaphoreType.DMA((n,)),
            pltpu.SemaphoreType.DMA((5,)),
            pltpu.SemaphoreType.DMA((5,)),
            pltpu.SemaphoreType.REGULAR,
        ],
        compiler_params=pltpu.CompilerParams(collective_id=0, has_side_effects=True),
    )(
        factor_b,
        factor_c,
        sample_j.reshape(n, 1, chunk),
        sample_k,
        sample_weight.reshape(n, 1, chunk),
        block_values.reshape(blocks, tile_rows),
        block_sample[0].transpose(1, 2, 0),
        block_count[0].transpose(1, 2, 0),
    )
    return factor_new, scales.reshape(rank)


def solution(mesh):
    in_specs = (
        P(None, ("groups", "row")),
        P(None, ("groups", "row")),
        P(("groups", "row")),
        P(None, ("groups", "row"), None),
        P(("groups", "row")),
        P(("groups", "row"), None, None, None, None),
        P(("groups", "row"), None, None, None),
        P(("groups", "row"), None, None, None),
    )
    out_specs = (P(None, ("groups", "row")), P("groups"))
    return jax.shard_map(shards, mesh=mesh, in_specs=in_specs, out_specs=out_specs, check_vma=False)
```

```python
import functools

import jax
import jax.numpy as jnp
from jax import lax
from jax.experimental import pallas as pl
from jax.experimental.pallas import tpu as pltpu
from jax.sharding import PartitionSpec as P

NN = (((1,), (0,)), ((), ()))
NT = (((1,), (1,)), ((), ()))
TN = (((0,), (0,)), ((), ()))
MESH = pl.DeviceIdType.MESH
UNROLLED_PEERS = 16
PANEL = 8


def pick_columns(folded, index, rank):
    width = folded.shape[1]
    count = index.shape[1]
    low = lax.rem(index, width)
    high = lax.div(index, width)
    rows = lax.broadcasted_iota(jnp.int16, (width, count), 0)
    one_hot = jnp.where(rows == low.astype(jnp.int16), jnp.bfloat16(1), jnp.bfloat16(0))
    products = jnp.dot(folded[...], one_hot, preferred_element_type=jnp.float32)
    picked = products[:rank]
    high = jnp.broadcast_to(high, (rank, count))
    for part in range(1, folded.shape[0] // rank):
        picked = jnp.where(high == part, products[part * rank : (part + 1) * rank], picked)
    return picked


def block_column(table_ref):
    table = jnp.concatenate([table_ref[tile] for tile in range(table_ref.shape[0])], axis=0)
    return jnp.concatenate(
        [table[:, peer : peer + 1] for peer in range(table.shape[1])], axis=0
    )


def product(left, right, dimensions=NT):
    return lax.dot_general(
        left,
        right,
        dimensions,
        precision=lax.Precision.HIGHEST,
        preferred_element_type=jnp.float32,
    )


def inverse(matrix):
    order = matrix.shape[0]
    lanes = lax.broadcasted_iota(jnp.int32, (8, order), 1)
    rows = lax.broadcasted_iota(jnp.int32, (8, order), 0)
    blocks = [matrix[first : first + 8] for first in range(0, order, 8)]
    for first in range(0, order, PANEL):
        panel = [
            [jnp.broadcast_to(block[:, k : k + 1], block.shape) for block in blocks]
            for k in range(first, first + PANEL)
        ]
        for step in range(PANEL):
            k = first + step
            home, place = divmod(k, 8)
            column = panel[step]
            pivot = 1.0 / column[home][place : place + 1]
            scaled = jnp.where(lanes[:1] == k, 1.0, blocks[home][place : place + 1]) * pivot
            blocks = [
                jnp.where(lanes == k, 0.0, block) - part * scaled
                for block, part in zip(blocks, column)
            ]
            blocks[home] = jnp.where(rows == place, scaled, blocks[home])
            for later in range(step + 1, PANEL):
                factor = panel[later][home][place : place + 1] * pivot
                panel[later] = [
                    block - part * factor for block, part in zip(panel[later], column)
                ]
                panel[later][home] = jnp.where(rows == place, factor, panel[later][home])
    return jnp.concatenate(blocks, axis=0)


def kernel(
    n,
    tiles,
    slots,
    total_rows,
    total_samples,
    b_hbm,
    c_hbm,
    j_hbm,
    k_hbm,
    w_hbm,
    values_hbm,
    sample_hbm,
    count_hbm,
    out_ref,
    scales_ref,
    folded_b,
    folded_c,
    j_ref,
    k_ref,
    w_ref,
    values_ref,
    sample_ref,
    count_ref,
    c_out,
    c_in,
    b_weighted,
    values_out,
    values_in,
    spread_ref,
    picks_out,
    picks_in,
    gram_out,
    gram_in,
    share_out,
    share_in,
    sample_column,
    moment_out,
    moment_in,
    load_sems,
    c_send,
    c_recv,
    send_sems,
    recv_sems,
    turn_sem,
):
    me = lax.axis_index("row")
    rank, b_rows = b_hbm.shape
    c_rows = c_hbm.shape[1]
    width = folded_c.shape[1]
    per_peer = tiles * slots
    blocks = n * per_peer
    chunk = c_in.shape[2]
    quarter = n // 4
    own = me // quarter
    place = me % quarter
    side = own // 2
    inner = (own + side) % 2

    def member(frame, turn):
        return (frame + side * (3 - 2 * frame)) * quarter + (place + turn) % quarter

    def sibling(turn):
        return own * quarter + (place + turn) % quarter

    def send_turn(turn):
        block = turn // quarter
        first, last = (2 - block) // 2, block // 2
        middle = 1 - first - last
        swap = inner * ((quarter - turn % quarter) // quarter) * (middle - first)
        first, middle = first + swap, middle - swap
        frame = first * (2 - 2 * inner) + middle * 3 + last * (1 + inner)
        return member(frame, turn % quarter)

    def late_turn(turn):
        block = turn // quarter
        return member((1 - block) * (3 - 3 * inner) + block * 2, quarter - turn % quarter)

    def loop(start, stop, body):
        if n <= UNROLLED_PEERS:
            for turn in range(start, stop):
                body(turn)
        else:
            lax.fori_loop(start, stop, lambda turn, carry: (body(turn), carry)[1], 0)

    def each_peer(body):
        for frame in (3, 2, 1 - inner):
            loop(0, quarter, lambda turn, frame=frame: body(member(frame, turn)))
        loop(1, quarter, lambda turn: body(sibling(turn)))

    def remote(peer, source, target, send, recv):
        return pltpu.make_async_remote_copy(
            src_ref=source,
            dst_ref=target,
            send_sem=send,
            recv_sem=recv,
            device_id={"row": peer},
            device_id_type=MESH,
        )

    def copy_c(peer, slot):
        return remote(peer, c_out.at[peer], c_in.at[slot], c_send.at[peer], c_recv.at[slot])

    def others(kind, target):
        region = target.at[pl.ds(0, n - 1)]
        return remote(sibling(1), region, region, send_sems.at[kind], recv_sems.at[kind])

    def spread_out(source, target, kind):
        each_peer(
            lambda peer: remote(
                peer, source.at[peer], target.at[me], send_sems.at[kind], recv_sems.at[kind]
            ).start()
        )

    def broadcast(source, target, kind):
        each_peer(
            lambda peer: remote(
                peer, source, target.at[me], send_sems.at[kind], recv_sems.at[kind]
            ).start()
        )

    piece = gram_out.shape[1]
    fold = rank // (n * piece)

    def scatter(pair, source, target, kind):
        if fold == 2:
            upper = lax.broadcasted_iota(jnp.int32, (rank // 2, 2 * rank), 1) < rank
            pair = jnp.where(upper, pair[: rank // 2], pair[rank // 2 :])
        for part in range(n):
            source[part] = pair[part * piece : (part + 1) * piece]
        target[me] = source[me]
        spread_out(source, target, kind)

    def gather(arrived, source, target, kind):
        source[...] = jnp.sum(arrived[...], axis=0)
        target[me] = source[...]
        broadcast(source, target, kind)

    def whole(arrived):
        matrix = jnp.concatenate([arrived[part] for part in range(n)], axis=0)
        if fold == 2:
            return jnp.concatenate([matrix[:, :rank], matrix[:, rank:]], axis=0)
        return matrix[:, :rank]

    barrier = pltpu.get_barrier_semaphore()
    each_peer(
        lambda peer: pl.semaphore_signal(
            barrier, inc=1, device_id={"row": peer}, device_id_type=MESH
        )
    )

    def load_table(source, target, kind):
        return [
            pltpu.make_async_copy(
                source.at[:, pl.ds(part * width, width)],
                target.at[pl.ds(part * rank, rank)],
                load_sems.at[kind],
            )
            for part in range(source.shape[1] // width)
        ]

    load_c = load_table(c_hbm, folded_c, 0)
    load_b = load_table(b_hbm, folded_b, 1)
    load_k = pltpu.make_async_copy(k_hbm, k_ref, load_sems.at[2])
    load_j = pltpu.make_async_copy(j_hbm, j_ref, load_sems.at[3])
    load_w = pltpu.make_async_copy(w_hbm, w_ref, load_sems.at[4])
    load_values = pltpu.make_async_copy(values_hbm, values_ref, load_sems.at[5])
    load_sample = pltpu.make_async_copy(sample_hbm, sample_ref, load_sems.at[6])
    load_count = pltpu.make_async_copy(count_hbm, count_ref, load_sems.at[7])
    for load in [load_k, *load_c, load_count, load_values, load_sample, load_j, *load_b, load_w]:
        load.start()

    def pick_c(peer):
        return pick_columns(folded_c, k_ref[peer] - me * c_rows, rank).astype(jnp.bfloat16)

    load_k.wait()
    for load in load_c:
        load.wait()
    c_out[send_turn(0)] = pick_c(send_turn(0))
    load_count.wait()
    load_values.wait()
    lanes = lax.broadcasted_iota(jnp.int32, (blocks, 128), 1)
    counts = block_column(count_ref)
    live = lanes < counts
    masked = jnp.where(live, values_ref[...].astype(jnp.float32), 0.0).astype(jnp.bfloat16)
    values_out[...] = masked.reshape(values_out.shape)
    values_in[me] = values_out[me]
    live_local = jnp.sum(counts.astype(jnp.float32), axis=0, keepdims=True)
    pl.semaphore_wait(barrier, n - 1)
    copy_c(send_turn(0), me).start()

    def send_c(peer):
        c_out[peer] = pick_c(peer)
        copy_c(peer, me).start()

    def send_far(turn, carry):
        send_c(send_turn(turn))
        return carry

    def send_near(turn, carry):
        send_c(sibling(turn))
        return carry

    lax.fori_loop(1, 3 * quarter, send_far, 0)
    lax.fori_loop(1, quarter, send_near, 0)

    @pl.when(inner == 1)
    def _():
        spread_out(values_out, values_in, 0)

    c_in[me] = pick_c(me)
    load_j.wait()
    load_w.wait()
    load_sample.wait()
    for load in load_b:
        load.wait()

    def pick_b(part, carry):
        picked = pick_columns(folded_b, j_ref[part] - me * b_rows, rank)
        b_weighted[part] = w_ref[part] * picked
        return carry

    lax.fori_loop(0, n, pick_b, 0)
    columns = lax.broadcasted_iota(jnp.int32, (blocks, chunk), 1)
    sample_column[...] = block_column(sample_ref)

    def add_chunk(part, carry):
        gram, picks = carry
        weights = w_ref[part]
        sketch = b_weighted[part] * c_in[part].astype(jnp.float32)
        top = sketch.astype(jnp.bfloat16)
        rest = (sketch - top.astype(jnp.float32)).astype(jnp.bfloat16)
        both = jnp.concatenate([top, rest], axis=0)
        gram = gram + lax.dot_general(both, both, NT, preferred_element_type=jnp.float32)
        weighted = (weights * sketch).astype(jnp.bfloat16)
        chosen = columns == sample_column[...] - part * chunk
        chosen = jnp.where(chosen, 1.0, 0.0).astype(jnp.bfloat16)
        picks = picks + lax.dot_general(
            chosen, weighted, NT, preferred_element_type=jnp.float32
        )
        return gram, picks

    def add_peer(part, carry):
        copy_c(part, part).wait_recv()
        return add_chunk(part, carry)

    carry = (
        jnp.zeros((2 * rank, 2 * rank), jnp.float32),
        jnp.zeros((blocks, rank), jnp.float32),
    )
    carry = add_chunk(me, carry)
    carry = lax.fori_loop(
        0, quarter, lambda turn, carry: add_peer(member(1 + 2 * inner, quarter - turn), carry), carry
    )
    carry = lax.fori_loop(
        1, quarter, lambda turn, carry: add_peer(sibling(quarter - turn), carry), carry
    )

    def add_late(turn, carry):
        carry = add_peer(late_turn(turn), carry)

        @pl.when((inner == 1) & (turn == 3 * quarter // 2 - 1))
        def _():
            pl.semaphore_signal(
                turn_sem, inc=1, device_id={"row": member(0, 0)}, device_id_type=MESH
            )

        return carry

    gram, picks = lax.fori_loop(0, 2 * quarter, add_late, carry)

    @pl.when(inner == 0)
    def _():
        pl.semaphore_wait(turn_sem, 1)
        spread_out(values_out, values_in, 0)

    rows_half = per_peer // 2
    picks = picks.reshape(n, per_peer, rank)
    picks_out[...] = jnp.concatenate(
        [picks[:, :rows_half], picks[:, rows_half:]], axis=2
    ).astype(jnp.bfloat16)
    picks_in[me] = picks_out[me]
    spread_out(picks_out, picks_in, 2)

    pair = gram[:rank] + gram[rank:]
    pair = (pair + pltpu.roll(pair, rank, 1)) / total_samples
    pair_rows = lax.broadcasted_iota(jnp.int32, pair.shape, 0)
    pair_lanes = lax.broadcasted_iota(jnp.int32, pair.shape, 1)
    ridge = 0.05 * live_local / total_rows
    pair = pair + jnp.where(pair_lanes % rank == pair_rows, ridge, 0.0)
    scatter(pair, gram_out, gram_in, 1)

    others(0, values_in).wait_recv()
    arrived = values_in[...].astype(jnp.float32)
    tile_of = lax.broadcasted_iota(jnp.int32, (n * rows_half, 128), 0) % rows_half // slots
    for part in range(2):
        rows = arrived[:, part * rows_half : (part + 1) * rows_half, :].reshape(-1, 128)
        spread_ref[part] = jnp.concatenate(
            [jnp.where(tile_of == tile, rows, 0.0) for tile in range(tiles // 2)], axis=1
        ).astype(jnp.bfloat16)

    others(2, picks_in).wait_recv()
    arrived = picks_in[...].astype(jnp.float32).reshape(-1, 2 * rank).astype(jnp.bfloat16)
    gathered = jnp.concatenate(
        [
            lax.dot_general(arrived, spread_ref[part], TN, preferred_element_type=jnp.float32)[
                part * rank : (part + 1) * rank
            ]
            for part in range(2)
        ],
        axis=1,
    )
    others(1, gram_in).wait_recv()
    gather(gram_in, share_out, share_in, 3)

    part = rank // 2
    top = product(gathered[:part], jnp.concatenate([gathered] * 2, axis=0))
    low = product(gathered[part:], jnp.concatenate([gathered[part:]] * 4, axis=0))
    rows = lax.broadcasted_iota(jnp.int32, (part, 2 * rank), 0)
    lanes = lax.broadcasted_iota(jnp.int32, (part, 2 * rank), 1)
    across = lanes % rank
    triangle = jnp.where(across >= rows, jnp.where(across == rows, top, 2.0 * top), 2.0 * low)
    quarter_rows = part // 2
    moment_out[:quarter_rows] = jnp.where(
        lanes[:quarter_rows] < rank, triangle[:quarter_rows], triangle[quarter_rows:]
    )
    moment_out[quarter_rows:] = jnp.sum(
        jnp.where(lanes == rows, low, 0.0), axis=0, keepdims=True
    )
    moment_in[me] = moment_out[...]
    broadcast(moment_out, moment_in, 4)

    others(3, share_in).wait_recv()
    inverted = inverse(whole(share_in))
    update = product(inverted, gathered, NN)
    first = jnp.concatenate([inverted] * 2, axis=1)
    second = jnp.concatenate([inverted[:, part:]] * 4, axis=1)
    others(4, moment_in).wait_recv()
    moment = jnp.sum(moment_in[...], axis=0)
    triangle, corner = moment[:quarter_rows], moment[quarter_rows:]
    above = across >= rows
    stacked = jnp.concatenate([triangle] * 2, axis=0)
    stacked = jnp.where((lanes < rank) == (rows < quarter_rows), stacked, 0.0)
    zeros = jnp.zeros_like(stacked)
    stacked = jnp.concatenate(
        [
            jnp.concatenate([jnp.where(above, stacked, 0.0), zeros], axis=1),
            jnp.concatenate([zeros, jnp.where(above, 0.0, stacked)], axis=1),
        ],
        axis=0,
    )
    solved = product(inverted, stacked, NN)
    squares = jnp.sum(
        solved[:, : 2 * rank] * first
        + solved[:, 2 * rank :] * second
        + corner * second * second,
        axis=1,
        keepdims=True,
    )
    scales = jnp.sqrt(jnp.maximum(squares, 0.0) / total_rows + 1e-06)
    out_ref[...] = (update / scales).astype(out_ref.dtype)
    diagonal = lax.broadcasted_iota(jnp.int32, (rank, rank), 0)
    diagonal = diagonal == lax.broadcasted_iota(jnp.int32, (rank, rank), 1)
    scales_ref[...] = jnp.sum(jnp.where(diagonal, scales, 0.0), axis=0, keepdims=True)

    each_peer(lambda peer: copy_c(peer, me).wait_send())
    others(0, values_out).wait_send()
    others(1, gram_out).wait_send()
    others(2, picks_out).wait_send()
    others(3, share_in).wait_send()
    others(4, moment_in).wait_send()


def shards(
    factor_b, factor_c, sample_j, sample_k, sample_weight, block_values, block_sample, block_count
):
    rank, b_rows = factor_b.shape
    n, _, chunk = sample_k.shape
    _, _, tiles, slots, tile_rows = block_values.shape
    samples = sample_j.shape[0]
    per_peer = tiles * slots
    blocks = n * per_peer
    width = 512
    piece = max(rank // (2 * n), 1)
    bf16, f32, i32 = jnp.bfloat16, jnp.float32, jnp.int32
    hbm = pl.BlockSpec(memory_space=pltpu.HBM)
    vmem = pl.BlockSpec(memory_space=pltpu.VMEM)
    factor_new, scales = pl.pallas_call(
        functools.partial(kernel, n, tiles, slots, tiles * tile_rows * n, samples * n),
        out_shape=(
            pltpu.VMEM((rank, tiles * tile_rows), bf16),
            pltpu.VMEM((1, rank), f32),
        ),
        in_specs=[hbm] * 8,
        out_specs=(vmem, vmem),
        scratch_shapes=[
            pltpu.VMEM((b_rows // width * rank, width), bf16),
            pltpu.VMEM((factor_c.shape[1] // width * rank, width), bf16),
            pltpu.VMEM((n, 1, chunk), i32),
            pltpu.VMEM((n, 1, chunk), i32),
            pltpu.VMEM((n, 1, chunk), f32),
            pltpu.VMEM((blocks, tile_rows), bf16),
            pltpu.VMEM((tiles, slots, n), i32),
            pltpu.VMEM((tiles, slots, n), i32),
            pltpu.VMEM((n, rank, chunk), bf16),
            pltpu.VMEM((n, rank, chunk), bf16),
            pltpu.VMEM((n, rank, chunk), f32),
            pltpu.VMEM((n, per_peer, tile_rows), bf16),
            pltpu.VMEM((n, per_peer, tile_rows), bf16),
            pltpu.VMEM((2, blocks // 2, tiles // 2 * tile_rows), bf16),
            pltpu.VMEM((n, per_peer // 2, 2 * rank), bf16),
            pltpu.VMEM((n, per_peer // 2, 2 * rank), bf16),
            pltpu.VMEM((n, piece, 2 * rank), f32),
            pltpu.VMEM((n, piece, 2 * rank), f32),
            pltpu.VMEM((piece, 2 * rank), f32),
            pltpu.VMEM((n, piece, 2 * rank), f32),
            pltpu.VMEM((blocks, 1), i32),
            pltpu.VMEM((rank // 4 + 1, 2 * rank), f32),
            pltpu.VMEM((n, rank // 4 + 1, 2 * rank), f32),
            pltpu.SemaphoreType.DMA((8,)),
            pltpu.SemaphoreType.DMA((n,)),
            pltpu.SemaphoreType.DMA((n,)),
            pltpu.SemaphoreType.DMA((5,)),
            pltpu.SemaphoreType.DMA((5,)),
            pltpu.SemaphoreType.REGULAR,
        ],
        compiler_params=pltpu.CompilerParams(collective_id=0, has_side_effects=True),
    )(
        factor_b,
        factor_c,
        sample_j.reshape(n, 1, chunk),
        sample_k,
        sample_weight.reshape(n, 1, chunk),
        block_values.reshape(blocks, tile_rows),
        block_sample[0].transpose(1, 2, 0),
        block_count[0].transpose(1, 2, 0),
    )
    return factor_new, scales.reshape(rank)


def solution(mesh):
    in_specs = (
        P(None, ("groups", "row")),
        P(None, ("groups", "row")),
        P(("groups", "row")),
        P(None, ("groups", "row"), None),
        P(("groups", "row")),
        P(("groups", "row"), None, None, None, None),
        P(("groups", "row"), None, None, None),
        P(("groups", "row"), None, None, None),
    )
    out_specs = (P(None, ("groups", "row")), P("groups"))
    return jax.shard_map(shards, mesh=mesh, in_specs=in_specs, out_specs=out_specs, check_vma=False)
```

```python
import functools

import jax
import jax.numpy as jnp
from jax import lax
from jax.experimental import pallas as pl
from jax.experimental.pallas import tpu as pltpu
from jax.sharding import PartitionSpec as P

NN = (((1,), (0,)), ((), ()))
NT = (((1,), (1,)), ((), ()))
TN = (((0,), (0,)), ((), ()))
MESH = pl.DeviceIdType.MESH
UNROLLED_PEERS = 16
PANEL = 8


def pick_columns(folded, index, rank):
    width = folded.shape[1]
    count = index.shape[1]
    low = lax.rem(index, width)
    high = lax.div(index, width)
    rows = lax.broadcasted_iota(jnp.int16, (width, count), 0)
    one_hot = jnp.where(rows == low.astype(jnp.int16), jnp.bfloat16(1), jnp.bfloat16(0))
    products = jnp.dot(folded[...], one_hot, preferred_element_type=jnp.float32)
    picked = products[:rank]
    high = jnp.broadcast_to(high, (rank, count))
    for part in range(1, folded.shape[0] // rank):
        picked = jnp.where(high == part, products[part * rank : (part + 1) * rank], picked)
    return picked


def block_column(table_ref):
    table = jnp.concatenate([table_ref[tile] for tile in range(table_ref.shape[0])], axis=0)
    return jnp.concatenate(
        [table[:, peer : peer + 1] for peer in range(table.shape[1])], axis=0
    )


def product(left, right, dimensions=NT):
    return lax.dot_general(
        left,
        right,
        dimensions,
        precision=lax.Precision.HIGHEST,
        preferred_element_type=jnp.float32,
    )


def inverse(matrix):
    order = matrix.shape[0]
    lanes = lax.broadcasted_iota(jnp.int32, (8, order), 1)
    rows = lax.broadcasted_iota(jnp.int32, (8, order), 0)
    blocks = [matrix[first : first + 8] for first in range(0, order, 8)]
    for first in range(0, order, PANEL):
        panel = [
            [jnp.broadcast_to(block[:, k : k + 1], block.shape) for block in blocks]
            for k in range(first, first + PANEL)
        ]
        for step in range(PANEL):
            k = first + step
            home, place = divmod(k, 8)
            column = panel[step]
            pivot = 1.0 / column[home][place : place + 1]
            scaled = jnp.where(lanes[:1] == k, 1.0, blocks[home][place : place + 1]) * pivot
            blocks = [
                jnp.where(lanes == k, 0.0, block) - part * scaled
                for block, part in zip(blocks, column)
            ]
            blocks[home] = jnp.where(rows == place, scaled, blocks[home])
            for later in range(step + 1, PANEL):
                factor = panel[later][home][place : place + 1] * pivot
                panel[later] = [
                    block - part * factor for block, part in zip(panel[later], column)
                ]
                panel[later][home] = jnp.where(rows == place, factor, panel[later][home])
    return jnp.concatenate(blocks, axis=0)


def kernel(
    n,
    tiles,
    slots,
    total_rows,
    total_samples,
    b_hbm,
    c_hbm,
    j_hbm,
    k_hbm,
    w_hbm,
    values_hbm,
    sample_hbm,
    count_hbm,
    update_ref,
    squares_ref,
    folded_b,
    folded_c,
    j_ref,
    k_ref,
    w_ref,
    values_ref,
    sample_ref,
    count_ref,
    c_out,
    c_in,
    b_weighted,
    values_out,
    values_in,
    spread_ref,
    picks_out,
    picks_in,
    gram_out,
    gram_in,
    share_out,
    share_in,
    sample_column,
    moment_out,
    moment_in,
    load_sems,
    c_recv,
    send_sem,
    recv_sems,
    turn_sem,
):
    me = lax.axis_index("row")
    rank, b_rows = b_hbm.shape
    c_rows = c_hbm.shape[1]
    width = folded_c.shape[1]
    per_peer = tiles * slots
    blocks = n * per_peer
    chunk = c_in.shape[2]
    quarter = n // 4
    own = me // quarter
    place = me % quarter
    side = own // 2
    inner = (own + side) % 2

    def member(frame, turn):
        return (frame + side * (3 - 2 * frame)) * quarter + (place + turn) % quarter

    def sibling(turn):
        return own * quarter + (place + turn) % quarter

    def send_turn(turn):
        block = turn // quarter
        first, last = (2 - block) // 2, block // 2
        middle = 1 - first - last
        swap = inner * ((quarter - turn % quarter) // quarter) * (middle - first)
        first, middle = first + swap, middle - swap
        frame = first * (2 - 2 * inner) + middle * 3 + last * (1 + inner)
        return member(frame, turn % quarter)

    def late_turn(turn):
        block = turn // quarter
        return member((1 - block) * (3 - 3 * inner) + block * 2, quarter - turn % quarter)

    def loop(start, stop, body):
        if n <= UNROLLED_PEERS:
            for turn in range(start, stop):
                body(turn)
        else:
            lax.fori_loop(start, stop, lambda turn, carry: (body(turn), carry)[1], 0)

    def each_peer(body):
        for frame in (3, 2, 1 - inner):
            loop(0, quarter, lambda turn, frame=frame: body(member(frame, turn)))
        loop(1, quarter, lambda turn: body(sibling(turn)))

    def remote(peer, source, target, send, recv):
        return pltpu.make_async_remote_copy(
            src_ref=source,
            dst_ref=target,
            send_sem=send,
            recv_sem=recv,
            device_id={"row": peer},
            device_id_type=MESH,
        )

    def copy_c(peer, slot):
        return remote(peer, c_out.at[peer], c_in.at[slot], send_sem, c_recv.at[slot])

    def others(kind, target):
        region = target.at[pl.ds(0, n - 1)]
        return remote(sibling(1), region, region, send_sem, recv_sems.at[kind])

    def spread_out(source, target, kind):
        each_peer(
            lambda peer: remote(
                peer, source.at[peer], target.at[me], send_sem, recv_sems.at[kind]
            ).start()
        )

    def broadcast(source, target, kind):
        each_peer(
            lambda peer: remote(
                peer, source, target.at[me], send_sem, recv_sems.at[kind]
            ).start()
        )

    piece = gram_out.shape[1]
    fold = rank // (n * piece)

    def scatter(pair, source, target, kind):
        if fold == 2:
            upper = lax.broadcasted_iota(jnp.int32, (rank // 2, 2 * rank), 1) < rank
            pair = jnp.where(upper, pair[: rank // 2], pair[rank // 2 :])
        for part in range(n):
            source[part] = pair[part * piece : (part + 1) * piece]
        target[me] = source[me]
        spread_out(source, target, kind)

    def gather(arrived, source, target, kind):
        source[...] = jnp.sum(arrived[...], axis=0)
        target[me] = source[...]
        broadcast(source, target, kind)

    def whole(arrived):
        matrix = jnp.concatenate([arrived[part] for part in range(n)], axis=0)
        if fold == 2:
            return jnp.concatenate([matrix[:, :rank], matrix[:, rank:]], axis=0)
        return matrix[:, :rank]

    barrier = pltpu.get_barrier_semaphore()
    each_peer(
        lambda peer: pl.semaphore_signal(
            barrier, inc=1, device_id={"row": peer}, device_id_type=MESH
        )
    )

    def load_table(source, target, kind):
        return [
            pltpu.make_async_copy(
                source.at[:, pl.ds(part * width, width)],
                target.at[pl.ds(part * rank, rank)],
                load_sems.at[kind],
            )
            for part in range(source.shape[1] // width)
        ]

    def load(source, target, kind):
        return [pltpu.make_async_copy(source, target, load_sems.at[kind])]

    loads = [
        load(k_hbm, k_ref, 0) + load_table(c_hbm, folded_c, 0),
        load(count_hbm, count_ref, 1)
        + load(values_hbm, values_ref, 1)
        + load(sample_hbm, sample_ref, 1),
        load(j_hbm, j_ref, 2) + load(w_hbm, w_ref, 2) + load_table(b_hbm, folded_b, 2),
    ]
    for copies in loads:
        for copy in copies:
            copy.start()

    def loaded(kind):
        for copy in loads[kind]:
            copy.wait()

    def pick_c(peer):
        return pick_columns(folded_c, k_ref[peer] - me * c_rows, rank).astype(jnp.bfloat16)

    loaded(0)
    c_out[send_turn(0)] = pick_c(send_turn(0))
    loaded(1)
    lanes = lax.broadcasted_iota(jnp.int32, (blocks, 128), 1)
    counts = block_column(count_ref)
    live = lanes < counts
    masked = jnp.where(live, values_ref[...].astype(jnp.float32), 0.0).astype(jnp.bfloat16)
    values_out[...] = masked.reshape(values_out.shape)
    values_in[me] = values_out[me]
    live_local = jnp.sum(counts.astype(jnp.float32), axis=0, keepdims=True)
    pl.semaphore_wait(barrier, n - 1)
    copy_c(send_turn(0), me).start()

    def send_c(peer):
        c_out[peer] = pick_c(peer)
        copy_c(peer, me).start()

    def send_far(turn, carry):
        send_c(send_turn(turn))
        return carry

    def send_near(turn, carry):
        send_c(sibling(turn))
        return carry

    lax.fori_loop(1, 3 * quarter, send_far, 0)
    lax.fori_loop(1, quarter, send_near, 0)

    @pl.when(inner == 1)
    def _():
        spread_out(values_out, values_in, 0)

    c_in[me] = pick_c(me)
    loaded(2)

    def pick_b(part, carry):
        picked = pick_columns(folded_b, j_ref[part] - me * b_rows, rank)
        b_weighted[part] = w_ref[part] * picked
        return carry

    lax.fori_loop(0, n, pick_b, 0)
    columns = lax.broadcasted_iota(jnp.int32, (blocks, chunk), 1)
    sample_column[...] = block_column(sample_ref)

    def add_chunk(part, carry):
        gram, picks = carry
        weights = w_ref[part]
        sketch = b_weighted[part] * c_in[part].astype(jnp.float32)
        top = sketch.astype(jnp.bfloat16)
        rest = (sketch - top.astype(jnp.float32)).astype(jnp.bfloat16)
        both = jnp.concatenate([top, rest], axis=0)
        gram = gram + lax.dot_general(both, both, NT, preferred_element_type=jnp.float32)
        weighted = (weights * sketch).astype(jnp.bfloat16)
        chosen = columns == sample_column[...] - part * chunk
        chosen = jnp.where(chosen, 1.0, 0.0).astype(jnp.bfloat16)
        picks = picks + lax.dot_general(
            chosen, weighted, NT, preferred_element_type=jnp.float32
        )
        return gram, picks

    def add_peer(part, carry):
        copy_c(part, part).wait_recv()
        return add_chunk(part, carry)

    carry = (
        jnp.zeros((2 * rank, 2 * rank), jnp.float32),
        jnp.zeros((blocks, rank), jnp.float32),
    )
    carry = add_chunk(me, carry)
    carry = lax.fori_loop(
        0, quarter, lambda turn, carry: add_peer(member(1 + 2 * inner, quarter - turn), carry), carry
    )
    carry = lax.fori_loop(
        1, quarter, lambda turn, carry: add_peer(sibling(quarter - turn), carry), carry
    )

    def add_late(turn, carry):
        carry = add_peer(late_turn(turn), carry)

        @pl.when((inner == 1) & (turn == 3 * quarter // 2 - 1))
        def _():
            pl.semaphore_signal(
                turn_sem, inc=1, device_id={"row": member(0, 0)}, device_id_type=MESH
            )

        return carry

    gram, picks = lax.fori_loop(0, 2 * quarter, add_late, carry)

    @pl.when(inner == 0)
    def _():
        pl.semaphore_wait(turn_sem, 1)
        spread_out(values_out, values_in, 0)

    pair = gram[:rank] + gram[rank:]
    pair = (pair + pltpu.roll(pair, rank, 1)) / total_samples
    pair_rows = lax.broadcasted_iota(jnp.int32, pair.shape, 0)
    pair_lanes = lax.broadcasted_iota(jnp.int32, pair.shape, 1)
    ridge = 0.05 * live_local / total_rows
    pair = pair + jnp.where(pair_lanes % rank == pair_rows, ridge, 0.0)
    scatter(pair, gram_out, gram_in, 1)

    rows_half = per_peer // 2
    picks = picks.reshape(n, per_peer, rank)
    picks_out[...] = jnp.concatenate(
        [picks[:, :rows_half], picks[:, rows_half:]], axis=2
    ).astype(jnp.bfloat16)
    picks_in[me] = picks_out[me]
    spread_out(picks_out, picks_in, 2)

    others(0, values_in).wait_recv()
    arrived = values_in[...].astype(jnp.float32)
    tile_of = lax.broadcasted_iota(jnp.int32, (n * rows_half, 128), 0) % rows_half // slots
    for part in range(2):
        rows = arrived[:, part * rows_half : (part + 1) * rows_half, :].reshape(-1, 128)
        spread_ref[part] = jnp.concatenate(
            [jnp.where(tile_of == tile, rows, 0.0) for tile in range(tiles // 2)], axis=1
        ).astype(jnp.bfloat16)

    others(1, gram_in).wait_recv()
    gather(gram_in, share_out, share_in, 3)
    others(2, picks_in).wait_recv()
    arrived = picks_in[...].astype(jnp.float32).reshape(-1, 2 * rank).astype(jnp.bfloat16)
    gathered = jnp.concatenate(
        [
            lax.dot_general(arrived, spread_ref[part], TN, preferred_element_type=jnp.float32)[
                part * rank : (part + 1) * rank
            ]
            for part in range(2)
        ],
        axis=1,
    )
    part = rank // 2
    top = product(gathered[:part], jnp.concatenate([gathered] * 2, axis=0))
    low = product(gathered[part:], jnp.concatenate([gathered[part:]] * 4, axis=0))
    rows = lax.broadcasted_iota(jnp.int32, (part, 2 * rank), 0)
    lanes = lax.broadcasted_iota(jnp.int32, (part, 2 * rank), 1)
    across = lanes % rank
    triangle = jnp.where(across >= rows, jnp.where(across == rows, top, 2.0 * top), 2.0 * low)
    quarter_rows = part // 2
    moment_out[:quarter_rows] = jnp.where(
        lanes[:quarter_rows] < rank, triangle[:quarter_rows], triangle[quarter_rows:]
    )
    moment_out[quarter_rows:] = jnp.sum(
        jnp.where(lanes == rows, low, 0.0), axis=0, keepdims=True
    )
    moment_in[me] = moment_out[...]
    broadcast(moment_out, moment_in, 4)

    others(3, share_in).wait_recv()
    inverted = inverse(whole(share_in))
    first = jnp.concatenate([inverted] * 2, axis=1)
    second = jnp.concatenate([inverted[:, part:]] * 4, axis=1)
    others(4, moment_in).wait_recv()
    moment = jnp.sum(moment_in[...], axis=0)
    triangle, corner = moment[:quarter_rows], moment[quarter_rows:]
    above = across >= rows
    stacked = jnp.concatenate([triangle] * 2, axis=0)
    stacked = jnp.where((lanes < rank) == (rows < quarter_rows), stacked, 0.0)
    zeros = jnp.zeros_like(stacked)
    stacked = jnp.concatenate(
        [
            jnp.concatenate([jnp.where(above, stacked, 0.0), zeros], axis=1),
            jnp.concatenate([zeros, jnp.where(above, 0.0, stacked)], axis=1),
        ],
        axis=0,
    )
    both = product(inverted, jnp.concatenate([stacked, gathered], axis=1), NN)
    solved, update_ref[...] = both[:, : 4 * rank], both[:, 4 * rank :]
    squares = jnp.sum(
        solved[:, : 2 * rank] * first
        + solved[:, 2 * rank :] * second
        + corner * second * second,
        axis=1,
        keepdims=True,
    )
    squares_ref[...] = squares

    for sent in (c_out, values_out, gram_out, picks_out, share_in, moment_in):
        others(0, sent).wait_send()


def shards(
    factor_b, factor_c, sample_j, sample_k, sample_weight, block_values, block_sample, block_count
):
    rank, b_rows = factor_b.shape
    n, _, chunk = sample_k.shape
    _, _, tiles, slots, tile_rows = block_values.shape
    samples = sample_j.shape[0]
    per_peer = tiles * slots
    blocks = n * per_peer
    width = 512
    piece = max(rank // (2 * n), 1)
    bf16, f32, i32 = jnp.bfloat16, jnp.float32, jnp.int32
    hbm = pl.BlockSpec(memory_space=pltpu.HBM)
    vmem = pl.BlockSpec(memory_space=pltpu.VMEM)
    total_rows = tiles * tile_rows * n
    update, squares = pl.pallas_call(
        functools.partial(kernel, n, tiles, slots, total_rows, samples * n),
        out_shape=(
            pltpu.VMEM((rank, tiles * tile_rows), f32),
            pltpu.VMEM((rank, 1), f32),
        ),
        in_specs=[hbm] * 8,
        out_specs=(vmem, vmem),
        scratch_shapes=[
            pltpu.VMEM((b_rows // width * rank, width), bf16),
            pltpu.VMEM((factor_c.shape[1] // width * rank, width), bf16),
            pltpu.VMEM((n, 1, chunk), i32),
            pltpu.VMEM((n, 1, chunk), i32),
            pltpu.VMEM((n, 1, chunk), f32),
            pltpu.VMEM((blocks, tile_rows), bf16),
            pltpu.VMEM((tiles, slots, n), i32),
            pltpu.VMEM((tiles, slots, n), i32),
            pltpu.VMEM((n, rank, chunk), bf16),
            pltpu.VMEM((n, rank, chunk), bf16),
            pltpu.VMEM((n, rank, chunk), f32),
            pltpu.VMEM((n, per_peer, tile_rows), bf16),
            pltpu.VMEM((n, per_peer, tile_rows), bf16),
            pltpu.VMEM((2, blocks // 2, tiles // 2 * tile_rows), bf16),
            pltpu.VMEM((n, per_peer // 2, 2 * rank), bf16),
            pltpu.VMEM((n, per_peer // 2, 2 * rank), bf16),
            pltpu.VMEM((n, piece, 2 * rank), f32),
            pltpu.VMEM((n, piece, 2 * rank), f32),
            pltpu.VMEM((piece, 2 * rank), f32),
            pltpu.VMEM((n, piece, 2 * rank), f32),
            pltpu.VMEM((blocks, 1), i32),
            pltpu.VMEM((rank // 4 + 1, 2 * rank), f32),
            pltpu.VMEM((n, rank // 4 + 1, 2 * rank), f32),
            pltpu.SemaphoreType.DMA((3,)),
            pltpu.SemaphoreType.DMA((n,)),
            pltpu.SemaphoreType.DMA,
            pltpu.SemaphoreType.DMA((5,)),
            pltpu.SemaphoreType.REGULAR,
        ],
        compiler_params=pltpu.CompilerParams(collective_id=0, has_side_effects=True),
    )(
        factor_b,
        factor_c,
        sample_j.reshape(n, 1, chunk),
        sample_k,
        sample_weight.reshape(n, 1, chunk),
        block_values.reshape(blocks, tile_rows),
        block_sample[0].transpose(1, 2, 0),
        block_count[0].transpose(1, 2, 0),
    )
    scales = jnp.sqrt(jnp.maximum(squares, 0.0) / total_rows + 1e-06)
    return (update / scales).astype(bf16), scales.reshape(rank)


def solution(mesh):
    in_specs = (
        P(None, ("groups", "row")),
        P(None, ("groups", "row")),
        P(("groups", "row")),
        P(None, ("groups", "row"), None),
        P(("groups", "row")),
        P(("groups", "row"), None, None, None, None),
        P(("groups", "row"), None, None, None),
        P(("groups", "row"), None, None, None),
    )
    out_specs = (P(None, ("groups", "row")), P("groups"))
    return jax.shard_map(shards, mesh=mesh, in_specs=in_specs, out_specs=out_specs, check_vma=False)
```

```python
import functools

import jax
import jax.numpy as jnp
from jax import lax
from jax.experimental import pallas as pl
from jax.experimental.pallas import tpu as pltpu
from jax.sharding import PartitionSpec as P

NT = (((1,), (1,)), ((), ()))
TN = (((0,), (0,)), ((), ()))
MESH = pl.DeviceIdType.MESH
UNROLLED_PEERS = 16
PANEL = 8


def pick_columns(folded, index, rank):
    width = folded.shape[1]
    count = index.shape[1]
    low = lax.rem(index, width)
    high = lax.div(index, width)
    rows = lax.broadcasted_iota(jnp.int16, (width, count), 0)
    one_hot = jnp.where(rows == low.astype(jnp.int16), jnp.bfloat16(1), jnp.bfloat16(0))
    products = jnp.dot(folded[...], one_hot, preferred_element_type=jnp.float32)
    picked = products[:rank]
    high = jnp.broadcast_to(high, (rank, count))
    for part in range(1, folded.shape[0] // rank):
        picked = jnp.where(high == part, products[part * rank : (part + 1) * rank], picked)
    return picked


def block_column(table_ref):
    table = jnp.concatenate([table_ref[tile] for tile in range(table_ref.shape[0])], axis=0)
    return jnp.concatenate(
        [table[:, peer : peer + 1] for peer in range(table.shape[1])], axis=0
    )


def product(left, right):
    return jnp.dot(
        left, right, precision=lax.Precision.HIGHEST, preferred_element_type=jnp.float32
    )


def halves(matrix):
    top = matrix.astype(jnp.bfloat16)
    return top, (matrix - top.astype(jnp.float32)).astype(jnp.bfloat16)


def inverse(matrix):
    order = matrix.shape[0]
    lanes = lax.broadcasted_iota(jnp.int32, (8, order), 1)
    rows = lax.broadcasted_iota(jnp.int32, (8, order), 0)
    blocks = [matrix[first : first + 8] for first in range(0, order, 8)]
    for first in range(0, order, PANEL):
        panel = [
            [jnp.broadcast_to(block[:, k : k + 1], block.shape) for block in blocks]
            for k in range(first, first + PANEL)
        ]
        for step in range(PANEL):
            k = first + step
            home, place = divmod(k, 8)
            column = panel[step]
            pivot = 1.0 / column[home][place : place + 1]
            scaled = jnp.where(lanes[:1] == k, 1.0, blocks[home][place : place + 1]) * pivot
            blocks = [
                jnp.where(lanes == k, 0.0, block) - part * scaled
                for block, part in zip(blocks, column)
            ]
            blocks[home] = jnp.where(rows == place, scaled, blocks[home])
            for later in range(step + 1, PANEL):
                factor = panel[later][home][place : place + 1] * pivot
                panel[later] = [
                    block - part * factor for block, part in zip(panel[later], column)
                ]
                panel[later][home] = jnp.where(rows == place, factor, panel[later][home])
    return jnp.concatenate(blocks, axis=0)


def kernel(
    n,
    tiles,
    slots,
    total_rows,
    total_samples,
    b_hbm,
    c_hbm,
    j_hbm,
    k_hbm,
    w_hbm,
    values_hbm,
    sample_hbm,
    count_hbm,
    update_ref,
    squares_ref,
    folded_b,
    folded_c,
    j_ref,
    k_ref,
    w_ref,
    values_ref,
    sample_ref,
    count_ref,
    c_out,
    c_in,
    b_weighted,
    values_out,
    values_in,
    spread_ref,
    picks_out,
    picks_in,
    gram_out,
    gram_in,
    share_out,
    share_in,
    sample_column,
    moment_out,
    moment_in,
    load_sems,
    c_recv,
    send_sem,
    recv_sems,
    turn_sem,
):
    me = lax.axis_index("row")
    rank, b_rows = b_hbm.shape
    c_rows = c_hbm.shape[1]
    width = folded_c.shape[1]
    per_peer = tiles * slots
    blocks = n * per_peer
    chunk = c_in.shape[2]
    quarter = n // 4
    own = me // quarter
    place = me % quarter
    side = own // 2
    inner = (own + side) % 2

    def member(frame, turn):
        return (frame + side * (3 - 2 * frame)) * quarter + (place + turn) % quarter

    def sibling(turn):
        return own * quarter + (place + turn) % quarter

    def send_turn(turn):
        block = turn // quarter
        first, last = (2 - block) // 2, block // 2
        middle = 1 - first - last
        swap = inner * ((quarter - turn % quarter) // quarter) * (middle - first)
        first, middle = first + swap, middle - swap
        frame = first * (2 - 2 * inner) + middle * 3 + last * (1 + inner)
        return member(frame, turn % quarter)

    def late_turn(turn):
        block = turn // quarter
        return member((1 - block) * (3 - 3 * inner) + block * 2, quarter - turn % quarter)

    def loop(start, stop, body):
        if n <= UNROLLED_PEERS:
            for turn in range(start, stop):
                body(turn)
        else:
            lax.fori_loop(start, stop, lambda turn, carry: (body(turn), carry)[1], 0)

    def each_peer(body):
        for frame in (3, 2, 1 - inner):
            loop(0, quarter, lambda turn, frame=frame: body(member(frame, turn)))
        loop(1, quarter, lambda turn: body(sibling(turn)))

    def remote(peer, source, target, send, recv):
        return pltpu.make_async_remote_copy(
            src_ref=source,
            dst_ref=target,
            send_sem=send,
            recv_sem=recv,
            device_id={"row": peer},
            device_id_type=MESH,
        )

    def copy_c(peer, slot):
        return remote(peer, c_out.at[peer], c_in.at[slot], send_sem, c_recv.at[slot])

    def others(kind, target):
        region = target.at[pl.ds(0, n - 1)]
        return remote(sibling(1), region, region, send_sem, recv_sems.at[kind])

    def spread_out(source, target, kind):
        each_peer(
            lambda peer: remote(
                peer, source.at[peer], target.at[me], send_sem, recv_sems.at[kind]
            ).start()
        )

    def broadcast(source, target, kind):
        each_peer(
            lambda peer: remote(
                peer, source, target.at[me], send_sem, recv_sems.at[kind]
            ).start()
        )

    piece = gram_out.shape[1]
    fold = rank // (n * piece)

    def scatter(pair, source, target, kind):
        if fold == 2:
            upper = lax.broadcasted_iota(jnp.int32, (rank // 2, 2 * rank), 1) < rank
            pair = jnp.where(upper, pair[: rank // 2], pair[rank // 2 :])
        for part in range(n):
            source[part] = pair[part * piece : (part + 1) * piece]
        target[me] = source[me]
        spread_out(source, target, kind)

    def gather(arrived, source, target, kind):
        source[...] = jnp.sum(arrived[...], axis=0)
        target[me] = source[...]
        broadcast(source, target, kind)

    def whole(arrived):
        matrix = jnp.concatenate([arrived[part] for part in range(n)], axis=0)
        if fold == 2:
            return jnp.concatenate([matrix[:, :rank], matrix[:, rank:]], axis=0)
        return matrix[:, :rank]

    barrier = pltpu.get_barrier_semaphore()
    each_peer(
        lambda peer: pl.semaphore_signal(
            barrier, inc=1, device_id={"row": peer}, device_id_type=MESH
        )
    )

    def load_table(source, target, kind):
        return [
            pltpu.make_async_copy(
                source.at[:, pl.ds(part * width, width)],
                target.at[pl.ds(part * rank, rank)],
                load_sems.at[kind],
            )
            for part in range(source.shape[1] // width)
        ]

    def load(source, target, kind):
        return [pltpu.make_async_copy(source, target, load_sems.at[kind])]

    loads = [
        load(k_hbm, k_ref, 0) + load_table(c_hbm, folded_c, 0),
        load(count_hbm, count_ref, 1)
        + load(values_hbm, values_ref, 1)
        + load(sample_hbm, sample_ref, 1),
        load(j_hbm, j_ref, 2) + load(w_hbm, w_ref, 2) + load_table(b_hbm, folded_b, 2),
    ]
    for copies in loads:
        for copy in copies:
            copy.start()

    def loaded(kind):
        for copy in loads[kind]:
            copy.wait()

    def pick_c(peer):
        return pick_columns(folded_c, k_ref[peer] - me * c_rows, rank).astype(jnp.bfloat16)

    loaded(0)
    c_out[send_turn(0)] = pick_c(send_turn(0))
    loaded(1)
    lanes = lax.broadcasted_iota(jnp.int32, (blocks, 128), 1)
    counts = block_column(count_ref)
    live = lanes < counts
    masked = jnp.where(live, values_ref[...].astype(jnp.float32), 0.0).astype(jnp.bfloat16)
    values_out[...] = masked.reshape(values_out.shape)
    values_in[me] = values_out[me]
    live_local = jnp.sum(counts.astype(jnp.float32), axis=0, keepdims=True)
    pl.semaphore_wait(barrier, n - 1)
    copy_c(send_turn(0), me).start()

    def send_c(peer):
        c_out[peer] = pick_c(peer)
        copy_c(peer, me).start()

    def send_far(turn, carry):
        send_c(send_turn(turn))
        return carry

    def send_near(turn, carry):
        send_c(sibling(turn))
        return carry

    lax.fori_loop(1, 3 * quarter, send_far, 0)
    lax.fori_loop(1, quarter, send_near, 0)

    @pl.when(inner == 1)
    def _():
        spread_out(values_out, values_in, 0)

    c_in[me] = pick_c(me)
    loaded(2)

    def pick_b(part, carry):
        picked = pick_columns(folded_b, j_ref[part] - me * b_rows, rank)
        b_weighted[part] = w_ref[part] * picked
        return carry

    lax.fori_loop(0, n, pick_b, 0)
    columns = lax.broadcasted_iota(jnp.int32, (blocks, chunk), 1)
    sample_column[...] = block_column(sample_ref)

    def add_chunk(part, carry):
        gram, picks = carry
        weights = w_ref[part]
        sketch = b_weighted[part] * c_in[part].astype(jnp.float32)
        both = jnp.concatenate(halves(sketch), axis=0)
        gram = gram + lax.dot_general(both, both, NT, preferred_element_type=jnp.float32)
        weighted = (weights * sketch).astype(jnp.bfloat16)
        chosen = columns == sample_column[...] - part * chunk
        chosen = jnp.where(chosen, 1.0, 0.0).astype(jnp.bfloat16)
        picks = picks + lax.dot_general(
            chosen, weighted, NT, preferred_element_type=jnp.float32
        )
        return gram, picks

    def add_peer(part, carry):
        copy_c(part, part).wait_recv()
        return add_chunk(part, carry)

    carry = (
        jnp.zeros((2 * rank, 2 * rank), jnp.float32),
        jnp.zeros((blocks, rank), jnp.float32),
    )
    carry = add_chunk(me, carry)
    carry = lax.fori_loop(
        0, quarter, lambda turn, carry: add_peer(member(1 + 2 * inner, quarter - turn), carry), carry
    )
    carry = lax.fori_loop(
        1, quarter, lambda turn, carry: add_peer(sibling(quarter - turn), carry), carry
    )

    def add_late(turn, carry):
        carry = add_peer(late_turn(turn), carry)

        @pl.when((inner == 1) & (turn == 3 * quarter // 2 - 1))
        def _():
            pl.semaphore_signal(
                turn_sem, inc=1, device_id={"row": member(0, 0)}, device_id_type=MESH
            )

        return carry

    gram, picks = lax.fori_loop(0, 2 * quarter, add_late, carry)

    @pl.when(inner == 0)
    def _():
        pl.semaphore_wait(turn_sem, 1)
        spread_out(values_out, values_in, 0)

    pair = gram[:rank] + gram[rank:]
    pair = (pair + pltpu.roll(pair, rank, 1)) / total_samples
    pair_rows = lax.broadcasted_iota(jnp.int32, pair.shape, 0)
    pair_lanes = lax.broadcasted_iota(jnp.int32, pair.shape, 1)
    ridge = 0.05 * live_local / total_rows
    pair = pair + jnp.where(pair_lanes % rank == pair_rows, ridge, 0.0)
    scatter(pair, gram_out, gram_in, 1)

    rows_half = per_peer // 2
    picks = picks.reshape(n, per_peer, rank)
    picks_out[...] = jnp.concatenate(
        [picks[:, :rows_half], picks[:, rows_half:]], axis=2
    ).astype(jnp.bfloat16)
    picks_in[me] = picks_out[me]
    spread_out(picks_out, picks_in, 2)

    others(0, values_in).wait_recv()
    arrived = values_in[...].astype(jnp.float32)
    tile_of = lax.broadcasted_iota(jnp.int32, (n * rows_half, 128), 0) % rows_half // slots
    for part in range(2):
        rows = arrived[:, part * rows_half : (part + 1) * rows_half, :].reshape(-1, 128)
        spread_ref[part] = jnp.concatenate(
            [jnp.where(tile_of == tile, rows, 0.0) for tile in range(tiles // 2)], axis=1
        ).astype(jnp.bfloat16)

    others(1, gram_in).wait_recv()
    gather(gram_in, share_out, share_in, 3)
    others(2, picks_in).wait_recv()
    arrived = picks_in[...].astype(jnp.float32).reshape(-1, 2 * rank).astype(jnp.bfloat16)
    gathered = jnp.concatenate(
        [
            lax.dot_general(arrived, spread_ref[part], TN, preferred_element_type=jnp.float32)[
                part * rank : (part + 1) * rank
            ]
            for part in range(2)
        ],
        axis=1,
    )
    part = rank // 2
    split = halves(gathered)
    columns = [jnp.concatenate([x] * 2 + [x[part:]] * 4, axis=0) for x in split]
    split = jnp.concatenate(split, axis=0)
    moments = sum(
        lax.dot_general(split, x, NT, preferred_element_type=jnp.float32) for x in columns
    )
    moments = moments[:rank] + moments[rank:]
    top, low = moments[:part, : 2 * rank], moments[part:, 2 * rank :]
    rows = lax.broadcasted_iota(jnp.int32, (part, 2 * rank), 0)
    lanes = lax.broadcasted_iota(jnp.int32, (part, 2 * rank), 1)
    across = lanes % rank
    triangle = jnp.where(across >= rows, jnp.where(across == rows, top, 2.0 * top), 2.0 * low)
    quarter_rows = part // 2
    moment_out[:quarter_rows] = jnp.where(
        lanes[:quarter_rows] < rank, triangle[:quarter_rows], triangle[quarter_rows:]
    )
    moment_out[quarter_rows:] = jnp.sum(
        jnp.where(lanes == rows, low, 0.0), axis=0, keepdims=True
    )
    moment_in[me] = moment_out[...]
    broadcast(moment_out, moment_in, 4)

    others(3, share_in).wait_recv()
    inverted = inverse(whole(share_in))
    first = jnp.concatenate([inverted] * 2, axis=1)
    second = jnp.concatenate([inverted[:, part:]] * 4, axis=1)
    others(4, moment_in).wait_recv()
    moment = jnp.sum(moment_in[...], axis=0)
    triangle, corner = moment[:quarter_rows], moment[quarter_rows:]
    above = across >= rows
    stacked = jnp.concatenate([triangle] * 2, axis=0)
    stacked = jnp.where((lanes < rank) == (rows < quarter_rows), stacked, 0.0)
    zeros = jnp.zeros_like(stacked)
    stacked = jnp.concatenate(
        [
            jnp.concatenate([jnp.where(above, stacked, 0.0), zeros], axis=1),
            jnp.concatenate([zeros, jnp.where(above, 0.0, stacked)], axis=1),
        ],
        axis=0,
    )
    both = product(inverted, jnp.concatenate([stacked, gathered], axis=1))
    solved, update_ref[...] = both[:, : 4 * rank], both[:, 4 * rank :]
    squares = jnp.sum(
        solved[:, : 2 * rank] * first
        + solved[:, 2 * rank :] * second
        + corner * second * second,
        axis=1,
        keepdims=True,
    )
    squares_ref[...] = squares

    for sent in (c_out, values_out, gram_out, picks_out, share_in, moment_in):
        others(0, sent).wait_send()


def shards(
    factor_b, factor_c, sample_j, sample_k, sample_weight, block_values, block_sample, block_count
):
    rank, b_rows = factor_b.shape
    n, _, chunk = sample_k.shape
    _, _, tiles, slots, tile_rows = block_values.shape
    samples = sample_j.shape[0]
    per_peer = tiles * slots
    blocks = n * per_peer
    width = 512
    piece = max(rank // (2 * n), 1)
    bf16, f32, i32 = jnp.bfloat16, jnp.float32, jnp.int32
    hbm = pl.BlockSpec(memory_space=pltpu.HBM)
    vmem = pl.BlockSpec(memory_space=pltpu.VMEM)
    total_rows = tiles * tile_rows * n
    update, squares = pl.pallas_call(
        functools.partial(kernel, n, tiles, slots, total_rows, samples * n),
        out_shape=(
            pltpu.VMEM((rank, tiles * tile_rows), f32),
            pltpu.VMEM((rank, 1), f32),
        ),
        in_specs=[hbm] * 8,
        out_specs=(vmem, vmem),
        scratch_shapes=[
            pltpu.VMEM((b_rows // width * rank, width), bf16),
            pltpu.VMEM((factor_c.shape[1] // width * rank, width), bf16),
            pltpu.VMEM((n, 1, chunk), i32),
            pltpu.VMEM((n, 1, chunk), i32),
            pltpu.VMEM((n, 1, chunk), f32),
            pltpu.VMEM((blocks, tile_rows), bf16),
            pltpu.VMEM((tiles, slots, n), i32),
            pltpu.VMEM((tiles, slots, n), i32),
            pltpu.VMEM((n, rank, chunk), bf16),
            pltpu.VMEM((n, rank, chunk), bf16),
            pltpu.VMEM((n, rank, chunk), f32),
            pltpu.VMEM((n, per_peer, tile_rows), bf16),
            pltpu.VMEM((n, per_peer, tile_rows), bf16),
            pltpu.VMEM((2, blocks // 2, tiles // 2 * tile_rows), bf16),
            pltpu.VMEM((n, per_peer // 2, 2 * rank), bf16),
            pltpu.VMEM((n, per_peer // 2, 2 * rank), bf16),
            pltpu.VMEM((n, piece, 2 * rank), f32),
            pltpu.VMEM((n, piece, 2 * rank), f32),
            pltpu.VMEM((piece, 2 * rank), f32),
            pltpu.VMEM((n, piece, 2 * rank), f32),
            pltpu.VMEM((blocks, 1), i32),
            pltpu.VMEM((rank // 4 + 1, 2 * rank), f32),
            pltpu.VMEM((n, rank // 4 + 1, 2 * rank), f32),
            pltpu.SemaphoreType.DMA((3,)),
            pltpu.SemaphoreType.DMA((n,)),
            pltpu.SemaphoreType.DMA,
            pltpu.SemaphoreType.DMA((5,)),
            pltpu.SemaphoreType.REGULAR,
        ],
        compiler_params=pltpu.CompilerParams(collective_id=0, has_side_effects=True),
    )(
        factor_b,
        factor_c,
        sample_j.reshape(n, 1, chunk),
        sample_k,
        sample_weight.reshape(n, 1, chunk),
        block_values.reshape(blocks, tile_rows),
        block_sample[0].transpose(1, 2, 0),
        block_count[0].transpose(1, 2, 0),
    )
    scales = jnp.sqrt(jnp.maximum(squares, 0.0) / total_rows + 1e-06)
    return (update / scales).astype(bf16), scales.reshape(rank)


def solution(mesh):
    in_specs = (
        P(None, ("groups", "row")),
        P(None, ("groups", "row")),
        P(("groups", "row")),
        P(None, ("groups", "row"), None),
        P(("groups", "row")),
        P(("groups", "row"), None, None, None, None),
        P(("groups", "row"), None, None, None),
        P(("groups", "row"), None, None, None),
    )
    out_specs = (P(None, ("groups", "row")), P("groups"))
    return jax.shard_map(shards, mesh=mesh, in_specs=in_specs, out_specs=out_specs, check_vma=False)
```

```python
import functools

import jax
import jax.numpy as jnp
from jax import lax
from jax.experimental import pallas as pl
from jax.experimental.pallas import tpu as pltpu
from jax.sharding import PartitionSpec as P

NT = (((1,), (1,)), ((), ()))
TN = (((0,), (0,)), ((), ()))
MESH = pl.DeviceIdType.MESH
UNROLLED_PEERS = 16
PANEL = 8


def pick_columns(folded, index, rank):
    width = folded.shape[1]
    count = index.shape[1]
    low = lax.rem(index, width)
    high = lax.div(index, width)
    rows = lax.broadcasted_iota(jnp.int16, (width, count), 0)
    one_hot = jnp.where(rows == low.astype(jnp.int16), jnp.bfloat16(1), jnp.bfloat16(0))
    products = jnp.dot(folded[...], one_hot, preferred_element_type=jnp.float32)
    picked = products[:rank]
    high = jnp.broadcast_to(high, (rank, count))
    for part in range(1, folded.shape[0] // rank):
        picked = jnp.where(high == part, products[part * rank : (part + 1) * rank], picked)
    return picked


def block_column(table_ref):
    table = jnp.concatenate([table_ref[tile] for tile in range(table_ref.shape[0])], axis=0)
    return jnp.concatenate(
        [table[:, peer : peer + 1] for peer in range(table.shape[1])], axis=0
    )


def product(left, right):
    return jnp.dot(
        left, right, precision=lax.Precision.HIGHEST, preferred_element_type=jnp.float32
    )


def halves(matrix):
    top = matrix.astype(jnp.bfloat16)
    return top, (matrix - top.astype(jnp.float32)).astype(jnp.bfloat16)


def inverse(matrix):
    order = matrix.shape[0]
    lanes = lax.broadcasted_iota(jnp.int32, (8, order), 1)
    rows = lax.broadcasted_iota(jnp.int32, (8, order), 0)
    blocks = [matrix[first : first + 8] for first in range(0, order, 8)]
    for first in range(0, order, PANEL):
        panel = [
            [jnp.broadcast_to(block[:, k : k + 1], block.shape) for block in blocks]
            for k in range(first, first + PANEL)
        ]
        for step in range(PANEL):
            k = first + step
            home, place = divmod(k, 8)
            column = panel[step]
            pivot = 1.0 / column[home][place : place + 1]
            scaled = jnp.where(lanes[:1] == k, 1.0, blocks[home][place : place + 1]) * pivot
            blocks = [
                jnp.where(lanes == k, 0.0, block) - part * scaled
                for block, part in zip(blocks, column)
            ]
            blocks[home] = jnp.where(rows == place, scaled, blocks[home])
            for later in range(step + 1, PANEL):
                factor = panel[later][home][place : place + 1] * pivot
                panel[later] = [
                    block - part * factor for block, part in zip(panel[later], column)
                ]
                panel[later][home] = jnp.where(rows == place, factor, panel[later][home])
    return jnp.concatenate(blocks, axis=0)


def kernel(
    n,
    tiles,
    slots,
    total_rows,
    total_samples,
    b_hbm,
    c_hbm,
    j_hbm,
    k_hbm,
    w_hbm,
    values_hbm,
    sample_hbm,
    count_hbm,
    update_ref,
    squares_ref,
    folded_b,
    folded_c,
    j_ref,
    k_ref,
    w_ref,
    values_ref,
    sample_ref,
    count_ref,
    c_out,
    c_in,
    b_weighted,
    values_out,
    values_in,
    spread_ref,
    picks_out,
    picks_in,
    gram_out,
    gram_in,
    share_out,
    share_in,
    sample_column,
    moment_out,
    moment_in,
    load_sems,
    c_recv,
    send_sem,
    recv_sems,
    turn_sem,
):
    me = lax.axis_index("row")
    rank, b_rows = b_hbm.shape
    c_rows = c_hbm.shape[1]
    width = folded_c.shape[1]
    per_peer = tiles * slots
    blocks = n * per_peer
    chunk = c_in.shape[2]
    quarter = n // 4
    own = me // quarter
    place = me % quarter
    side = own // 2
    inner = (own + side) % 2

    def member(frame, turn):
        return (frame + side * (3 - 2 * frame)) * quarter + (place + turn) % quarter

    def sibling(turn):
        return own * quarter + (place + turn) % quarter

    def send_turn(turn):
        block = turn // quarter
        first, last = (2 - block) // 2, block // 2
        middle = 1 - first - last
        swap = inner * ((quarter - turn % quarter) // quarter) * (middle - first)
        first, middle = first + swap, middle - swap
        frame = first * (2 - 2 * inner) + middle * 3 + last * (1 + inner)
        return member(frame, turn % quarter)

    def late_turn(turn):
        block = turn // quarter
        return member((1 - block) * (3 - 3 * inner) + block * 2, quarter - turn % quarter)

    def loop(start, stop, body):
        if n <= UNROLLED_PEERS:
            for turn in range(start, stop):
                body(turn)
        else:
            lax.fori_loop(start, stop, lambda turn, carry: (body(turn), carry)[1], 0)

    def each_peer(body):
        for frame in (3, 1 - inner):
            loop(0, quarter, lambda turn, frame=frame: body(member(frame, turn - place + quarter)))
        loop(1, quarter, lambda turn: body(sibling(turn)))
        loop(0, quarter, lambda turn: body(member(2, turn - place + quarter)))

    def remote(peer, source, target, send, recv):
        return pltpu.make_async_remote_copy(
            src_ref=source,
            dst_ref=target,
            send_sem=send,
            recv_sem=recv,
            device_id={"row": peer},
            device_id_type=MESH,
        )

    def copy_c(peer, slot):
        return remote(peer, c_out.at[peer], c_in.at[slot], send_sem, c_recv.at[slot])

    def others(kind, target):
        region = target.at[pl.ds(0, n - 1)]
        return remote(sibling(1), region, region, send_sem, recv_sems.at[kind])

    def spread_out(source, target, kind):
        each_peer(
            lambda peer: remote(
                peer, source.at[peer], target.at[me], send_sem, recv_sems.at[kind]
            ).start()
        )

    def broadcast(source, target, kind):
        each_peer(
            lambda peer: remote(
                peer, source, target.at[me], send_sem, recv_sems.at[kind]
            ).start()
        )

    piece = gram_out.shape[1]
    fold = rank // (n * piece)

    def scatter(pair, source, target, kind):
        if fold == 2:
            upper = lax.broadcasted_iota(jnp.int32, (rank // 2, 2 * rank), 1) < rank
            pair = jnp.where(upper, pair[: rank // 2], pair[rank // 2 :])
        for part in range(n):
            source[part] = pair[part * piece : (part + 1) * piece]
        target[me] = source[me]
        spread_out(source, target, kind)

    def gather(arrived, source, target, kind):
        source[...] = jnp.sum(arrived[...], axis=0)
        target[me] = source[...]
        broadcast(source, target, kind)

    def whole(arrived):
        matrix = jnp.concatenate([arrived[part] for part in range(n)], axis=0)
        if fold == 2:
            return jnp.concatenate([matrix[:, :rank], matrix[:, rank:]], axis=0)
        return matrix[:, :rank]

    barrier = pltpu.get_barrier_semaphore()
    each_peer(
        lambda peer: pl.semaphore_signal(
            barrier, inc=1, device_id={"row": peer}, device_id_type=MESH
        )
    )

    def load_table(source, target, kind):
        return [
            pltpu.make_async_copy(
                source.at[:, pl.ds(part * width, width)],
                target.at[pl.ds(part * rank, rank)],
                load_sems.at[kind],
            )
            for part in range(source.shape[1] // width)
        ]

    def load(source, target, kind):
        return [pltpu.make_async_copy(source, target, load_sems.at[kind])]

    loads = [
        load(k_hbm, k_ref, 0) + load_table(c_hbm, folded_c, 0),
        load(count_hbm, count_ref, 1)
        + load(values_hbm, values_ref, 1)
        + load(sample_hbm, sample_ref, 1),
        load(j_hbm, j_ref, 2) + load(w_hbm, w_ref, 2) + load_table(b_hbm, folded_b, 2),
    ]
    for copies in loads:
        for copy in copies:
            copy.start()

    def loaded(kind):
        for copy in loads[kind]:
            copy.wait()

    def pick_c(peer):
        return pick_columns(folded_c, k_ref[peer] - me * c_rows, rank).astype(jnp.bfloat16)

    loaded(0)
    c_out[send_turn(0)] = pick_c(send_turn(0))
    loaded(1)
    lanes = lax.broadcasted_iota(jnp.int32, (blocks, 128), 1)
    counts = block_column(count_ref)
    live = lanes < counts
    masked = jnp.where(live, values_ref[...].astype(jnp.float32), 0.0).astype(jnp.bfloat16)
    values_out[...] = masked.reshape(values_out.shape)
    values_in[me] = values_out[me]
    live_local = jnp.sum(counts.astype(jnp.float32), axis=0, keepdims=True)
    pl.semaphore_wait(barrier, n - 1)
    copy_c(send_turn(0), me).start()

    def send_c(peer):
        c_out[peer] = pick_c(peer)
        copy_c(peer, me).start()

    def send_far(turn, carry):
        send_c(send_turn(turn))
        return carry

    def send_near(turn, carry):
        send_c(sibling(turn))
        return carry

    lax.fori_loop(1, 3 * quarter, send_far, 0)
    lax.fori_loop(1, quarter, send_near, 0)

    @pl.when(inner == 1)
    def _():
        spread_out(values_out, values_in, 0)

    c_in[me] = pick_c(me)
    loaded(2)

    def pick_b(part, carry):
        picked = pick_columns(folded_b, j_ref[part] - me * b_rows, rank)
        b_weighted[part] = w_ref[part] * picked
        return carry

    lax.fori_loop(0, n, pick_b, 0)
    columns = lax.broadcasted_iota(jnp.int32, (blocks, chunk), 1)
    sample_column[...] = block_column(sample_ref)

    def add_chunk(part, carry):
        gram, picks = carry
        weights = w_ref[part]
        sketch = b_weighted[part] * c_in[part].astype(jnp.float32)
        both = jnp.concatenate(halves(sketch), axis=0)
        gram = gram + lax.dot_general(both, both, NT, preferred_element_type=jnp.float32)
        weighted = (weights * sketch).astype(jnp.bfloat16)
        chosen = columns == sample_column[...] - part * chunk
        chosen = jnp.where(chosen, 1.0, 0.0).astype(jnp.bfloat16)
        picks = picks + lax.dot_general(
            chosen, weighted, NT, preferred_element_type=jnp.float32
        )
        return gram, picks

    def add_peer(part, carry):
        copy_c(part, part).wait_recv()
        return add_chunk(part, carry)

    carry = (
        jnp.zeros((2 * rank, 2 * rank), jnp.float32),
        jnp.zeros((blocks, rank), jnp.float32),
    )
    carry = add_chunk(me, carry)
    carry = lax.fori_loop(
        0, quarter, lambda turn, carry: add_peer(member(1 + 2 * inner, quarter - turn), carry), carry
    )
    carry = lax.fori_loop(
        1, quarter, lambda turn, carry: add_peer(sibling(quarter - turn), carry), carry
    )

    def add_late(turn, carry):
        carry = add_peer(late_turn(turn), carry)

        @pl.when((inner == 1) & (turn == 3 * quarter // 2 - 1))
        def _():
            pl.semaphore_signal(
                turn_sem, inc=1, device_id={"row": member(0, 0)}, device_id_type=MESH
            )

        return carry

    gram, picks = lax.fori_loop(0, 2 * quarter, add_late, carry)

    @pl.when(inner == 0)
    def _():
        pl.semaphore_wait(turn_sem, 1)
        spread_out(values_out, values_in, 0)

    pair = gram[:rank] + gram[rank:]
    pair = (pair + pltpu.roll(pair, rank, 1)) / total_samples
    pair_rows = lax.broadcasted_iota(jnp.int32, pair.shape, 0)
    pair_lanes = lax.broadcasted_iota(jnp.int32, pair.shape, 1)
    ridge = 0.05 * live_local / total_rows
    pair = pair + jnp.where(pair_lanes % rank == pair_rows, ridge, 0.0)
    scatter(pair, gram_out, gram_in, 1)

    rows_half = per_peer // 2
    picks = picks.reshape(n, per_peer, rank)
    picks_out[...] = jnp.concatenate(
        [picks[:, :rows_half], picks[:, rows_half:]], axis=2
    ).astype(jnp.bfloat16)
    picks_in[me] = picks_out[me]
    spread_out(picks_out, picks_in, 2)

    others(0, values_in).wait_recv()
    arrived = values_in[...].astype(jnp.float32)
    tile_of = lax.broadcasted_iota(jnp.int32, (n * rows_half, 128), 0) % rows_half // slots
    for part in range(2):
        rows = arrived[:, part * rows_half : (part + 1) * rows_half, :].reshape(-1, 128)
        spread_ref[part] = jnp.concatenate(
            [jnp.where(tile_of == tile, rows, 0.0) for tile in range(tiles // 2)], axis=1
        ).astype(jnp.bfloat16)

    others(1, gram_in).wait_recv()
    gather(gram_in, share_out, share_in, 3)
    others(2, picks_in).wait_recv()
    arrived = picks_in[...].astype(jnp.float32).reshape(-1, 2 * rank).astype(jnp.bfloat16)
    gathered = jnp.concatenate(
        [
            lax.dot_general(arrived, spread_ref[part], TN, preferred_element_type=jnp.float32)[
                part * rank : (part + 1) * rank
            ]
            for part in range(2)
        ],
        axis=1,
    )
    part = rank // 2
    split = halves(gathered)
    columns = [jnp.concatenate([x] * 2 + [x[part:]] * 4, axis=0) for x in split]
    split = jnp.concatenate(split, axis=0)
    moments = sum(
        lax.dot_general(split, x, NT, preferred_element_type=jnp.float32) for x in columns
    )
    moments = moments[:rank] + moments[rank:]
    top, low = moments[:part, : 2 * rank], moments[part:, 2 * rank :]
    rows = lax.broadcasted_iota(jnp.int32, (part, 2 * rank), 0)
    lanes = lax.broadcasted_iota(jnp.int32, (part, 2 * rank), 1)
    across = lanes % rank
    triangle = jnp.where(across >= rows, jnp.where(across == rows, top, 2.0 * top), 2.0 * low)
    quarter_rows = part // 2
    moment_out[:quarter_rows] = jnp.where(
        lanes[:quarter_rows] < rank, triangle[:quarter_rows], triangle[quarter_rows:]
    )
    moment_out[quarter_rows:] = jnp.sum(
        jnp.where(lanes == rows, low, 0.0), axis=0, keepdims=True
    )
    moment_in[me] = moment_out[...]
    broadcast(moment_out, moment_in, 4)

    others(3, share_in).wait_recv()
    inverted = inverse(whole(share_in))
    first = jnp.concatenate([inverted] * 2, axis=1)
    second = jnp.concatenate([inverted[:, part:]] * 4, axis=1)
    others(4, moment_in).wait_recv()
    moment = jnp.sum(moment_in[...], axis=0)
    triangle, corner = moment[:quarter_rows], moment[quarter_rows:]
    above = across >= rows
    stacked = jnp.concatenate([triangle] * 2, axis=0)
    stacked = jnp.where((lanes < rank) == (rows < quarter_rows), stacked, 0.0)
    zeros = jnp.zeros_like(stacked)
    stacked = jnp.concatenate(
        [
            jnp.concatenate([jnp.where(above, stacked, 0.0), zeros], axis=1),
            jnp.concatenate([zeros, jnp.where(above, 0.0, stacked)], axis=1),
        ],
        axis=0,
    )
    both = product(inverted, jnp.concatenate([stacked, gathered], axis=1))
    solved, update_ref[...] = both[:, : 4 * rank], both[:, 4 * rank :]
    squares = jnp.sum(
        solved[:, : 2 * rank] * first
        + solved[:, 2 * rank :] * second
        + corner * second * second,
        axis=1,
        keepdims=True,
    )
    squares_ref[...] = squares

    for sent in (c_out, values_out, gram_out, picks_out, share_in, moment_in):
        others(0, sent).wait_send()


def shards(
    factor_b, factor_c, sample_j, sample_k, sample_weight, block_values, block_sample, block_count
):
    rank, b_rows = factor_b.shape
    n, _, chunk = sample_k.shape
    _, _, tiles, slots, tile_rows = block_values.shape
    samples = sample_j.shape[0]
    per_peer = tiles * slots
    blocks = n * per_peer
    width = 512
    piece = max(rank // (2 * n), 1)
    bf16, f32, i32 = jnp.bfloat16, jnp.float32, jnp.int32
    hbm = pl.BlockSpec(memory_space=pltpu.HBM)
    vmem = pl.BlockSpec(memory_space=pltpu.VMEM)
    total_rows = tiles * tile_rows * n
    update, squares = pl.pallas_call(
        functools.partial(kernel, n, tiles, slots, total_rows, samples * n),
        out_shape=(
            pltpu.VMEM((rank, tiles * tile_rows), f32),
            pltpu.VMEM((rank, 1), f32),
        ),
        in_specs=[hbm] * 8,
        out_specs=(vmem, vmem),
        scratch_shapes=[
            pltpu.VMEM((b_rows // width * rank, width), bf16),
            pltpu.VMEM((factor_c.shape[1] // width * rank, width), bf16),
            pltpu.VMEM((n, 1, chunk), i32),
            pltpu.VMEM((n, 1, chunk), i32),
            pltpu.VMEM((n, 1, chunk), f32),
            pltpu.VMEM((blocks, tile_rows), bf16),
            pltpu.VMEM((tiles, slots, n), i32),
            pltpu.VMEM((tiles, slots, n), i32),
            pltpu.VMEM((n, rank, chunk), bf16),
            pltpu.VMEM((n, rank, chunk), bf16),
            pltpu.VMEM((n, rank, chunk), f32),
            pltpu.VMEM((n, per_peer, tile_rows), bf16),
            pltpu.VMEM((n, per_peer, tile_rows), bf16),
            pltpu.VMEM((2, blocks // 2, tiles // 2 * tile_rows), bf16),
            pltpu.VMEM((n, per_peer // 2, 2 * rank), bf16),
            pltpu.VMEM((n, per_peer // 2, 2 * rank), bf16),
            pltpu.VMEM((n, piece, 2 * rank), f32),
            pltpu.VMEM((n, piece, 2 * rank), f32),
            pltpu.VMEM((piece, 2 * rank), f32),
            pltpu.VMEM((n, piece, 2 * rank), f32),
            pltpu.VMEM((blocks, 1), i32),
            pltpu.VMEM((rank // 4 + 1, 2 * rank), f32),
            pltpu.VMEM((n, rank // 4 + 1, 2 * rank), f32),
            pltpu.SemaphoreType.DMA((3,)),
            pltpu.SemaphoreType.DMA((n,)),
            pltpu.SemaphoreType.DMA,
            pltpu.SemaphoreType.DMA((5,)),
            pltpu.SemaphoreType.REGULAR,
        ],
        compiler_params=pltpu.CompilerParams(collective_id=0, has_side_effects=True),
    )(
        factor_b,
        factor_c,
        sample_j.reshape(n, 1, chunk),
        sample_k,
        sample_weight.reshape(n, 1, chunk),
        block_values.reshape(blocks, tile_rows),
        block_sample[0].transpose(1, 2, 0),
        block_count[0].transpose(1, 2, 0),
    )
    scales = jnp.sqrt(jnp.maximum(squares, 0.0) / total_rows + 1e-06)
    return (update / scales).astype(bf16), scales.reshape(rank)


def solution(mesh):
    in_specs = (
        P(None, ("groups", "row")),
        P(None, ("groups", "row")),
        P(("groups", "row")),
        P(None, ("groups", "row"), None),
        P(("groups", "row")),
        P(("groups", "row"), None, None, None, None),
        P(("groups", "row"), None, None, None),
        P(("groups", "row"), None, None, None),
    )
    out_specs = (P(None, ("groups", "row")), P("groups"))
    return jax.shard_map(shards, mesh=mesh, in_specs=in_specs, out_specs=out_specs, check_vma=False)
```

```python
import functools

import jax
import jax.numpy as jnp
from jax import lax
from jax.experimental import pallas as pl
from jax.experimental.pallas import tpu as pltpu
from jax.sharding import PartitionSpec as P

NT = (((1,), (1,)), ((), ()))
TN = (((0,), (0,)), ((), ()))
MESH = pl.DeviceIdType.MESH
UNROLLED_PEERS = 16


def pick_columns(folded, index, rank):
    width = folded.shape[1]
    count = index.shape[1]
    low = lax.rem(index, width)
    high = lax.div(index, width)
    rows = lax.broadcasted_iota(jnp.int16, (width, count), 0)
    one_hot = jnp.where(rows == low.astype(jnp.int16), jnp.bfloat16(1), jnp.bfloat16(0))
    products = jnp.dot(folded[...], one_hot, preferred_element_type=jnp.float32)
    picked = products[:rank]
    high = jnp.broadcast_to(high, (rank, count))
    for part in range(1, folded.shape[0] // rank):
        picked = jnp.where(high == part, products[part * rank : (part + 1) * rank], picked)
    return picked


def block_column(table_ref):
    table = jnp.concatenate([table_ref[tile] for tile in range(table_ref.shape[0])], axis=0)
    return jnp.concatenate(
        [table[:, peer : peer + 1] for peer in range(table.shape[1])], axis=0
    )


def product(left, right):
    return jnp.dot(
        left, right, precision=lax.Precision.HIGHEST, preferred_element_type=jnp.float32
    )


def halves(matrix):
    top = matrix.astype(jnp.bfloat16)
    return top, (matrix - top.astype(jnp.float32)).astype(jnp.bfloat16)


def inverse(matrix):
    order = matrix.shape[0]
    lanes = lax.broadcasted_iota(jnp.int32, (8, order), 1)
    rows = lax.broadcasted_iota(jnp.int32, (8, order), 0)
    blocks = [matrix[first : first + 8] for first in range(0, order, 8)]

    def spread(block, first):
        return [
            jnp.broadcast_to(block[:, k : k + 1], block.shape) for k in range(first, first + 8)
        ]

    own = spread(blocks[0], 0)
    for home in range(len(blocks)):
        first = 8 * home
        last = home + 1 == len(blocks)
        spreads = [
            own if place == home else spread(block, first) for place, block in enumerate(blocks)
        ]
        panel = [list(column) for column in zip(*spreads)]
        if not last:
            ahead = spread(blocks[home], first + 8)
            following = spread(blocks[home + 1], first + 8)
        for step in range(8):
            k = first + step
            column = panel[step]
            pivot = 1.0 / own[step][step : step + 1]
            scaled = jnp.where(lanes[:1] == k, 1.0, blocks[home][step : step + 1]) * pivot
            blocks = [
                jnp.where(lanes == k, 0.0, block) - part * scaled
                for block, part in zip(blocks, column)
            ]
            blocks[home] = jnp.where(rows == step, scaled, blocks[home])
            for later in range(step + 1, 8):
                factor = own[later][step : step + 1] * pivot
                own[later] = own[later] - own[step] * factor
                panel[later] = [
                    block - part * factor for block, part in zip(panel[later], column)
                ]
                panel[later][home] = jnp.where(rows == step, factor, panel[later][home])
            if not last:
                for later in range(8):
                    factor = ahead[later][step : step + 1] * pivot
                    ahead[later] = ahead[later] - own[step] * factor
                    following[later] = following[later] - column[home + 1] * factor
        if not last:
            own = following
    return jnp.concatenate(blocks, axis=0)


def kernel(
    n,
    tiles,
    slots,
    total_rows,
    total_samples,
    b_hbm,
    c_hbm,
    j_hbm,
    k_hbm,
    w_hbm,
    values_hbm,
    sample_hbm,
    count_hbm,
    update_ref,
    squares_ref,
    folded_b,
    folded_c,
    j_ref,
    k_ref,
    w_ref,
    values_ref,
    sample_ref,
    count_ref,
    c_out,
    c_in,
    b_weighted,
    values_out,
    values_in,
    spread_ref,
    picks_out,
    picks_in,
    gram_out,
    gram_in,
    share_out,
    share_in,
    sample_column,
    moment_out,
    moment_in,
    load_sems,
    c_recv,
    send_sem,
    recv_sems,
    turn_sem,
):
    me = lax.axis_index("row")
    rank, b_rows = b_hbm.shape
    c_rows = c_hbm.shape[1]
    width = folded_c.shape[1]
    per_peer = tiles * slots
    blocks = n * per_peer
    chunk = c_in.shape[2]
    quarter = n // 4
    own = me // quarter
    place = me % quarter
    side = own // 2
    inner = (own + side) % 2

    def member(frame, turn):
        return (frame + side * (3 - 2 * frame)) * quarter + (place + turn) % quarter

    def sibling(turn):
        return own * quarter + (place + turn) % quarter

    def send_turn(turn):
        block = turn // quarter
        first, last = (2 - block) // 2, block // 2
        middle = 1 - first - last
        swap = inner * ((quarter + 1 - turn % quarter) // quarter) * (middle - first)
        first, middle = first + swap, middle - swap
        frame = first * (2 - 2 * inner) + middle * 3 + last * (1 + inner)
        return member(frame, turn % quarter)

    def late_turn(turn):
        block = turn // quarter
        return member((1 - block) * (3 - 3 * inner) + block * 2, quarter - turn % quarter)

    def loop(start, stop, body):
        if n <= UNROLLED_PEERS:
            for turn in range(start, stop):
                body(turn)
        else:
            lax.fori_loop(start, stop, lambda turn, carry: (body(turn), carry)[1], 0)

    def each_peer(body):
        for frame in (3, 1 - inner):
            loop(0, quarter, lambda turn, frame=frame: body(member(frame, turn - place + quarter)))
        loop(1, quarter, lambda turn: body(sibling(turn)))
        loop(0, quarter, lambda turn: body(member(2, turn - place + quarter)))

    def remote(peer, source, target, send, recv):
        return pltpu.make_async_remote_copy(
            src_ref=source,
            dst_ref=target,
            send_sem=send,
            recv_sem=recv,
            device_id={"row": peer},
            device_id_type=MESH,
        )

    def copy_c(peer, slot):
        return remote(peer, c_out.at[peer], c_in.at[slot], send_sem, c_recv.at[slot])

    def others(kind, target):
        region = target.at[pl.ds(0, n - 1)]
        return remote(sibling(1), region, region, send_sem, recv_sems.at[kind])

    def spread_out(source, target, kind):
        each_peer(
            lambda peer: remote(
                peer, source.at[peer], target.at[me], send_sem, recv_sems.at[kind]
            ).start()
        )

    def broadcast(source, target, kind):
        each_peer(
            lambda peer: remote(
                peer, source, target.at[me], send_sem, recv_sems.at[kind]
            ).start()
        )

    piece = gram_out.shape[1]
    fold = rank // (n * piece)

    def scatter(pair, source, target, kind):
        if fold == 2:
            upper = lax.broadcasted_iota(jnp.int32, (rank // 2, 2 * rank), 1) < rank
            pair = jnp.where(upper, pair[: rank // 2], pair[rank // 2 :])
        for part in range(n):
            source[part] = pair[part * piece : (part + 1) * piece]
        target[me] = source[me]
        spread_out(source, target, kind)

    def gather(arrived, source, target, kind):
        source[...] = jnp.sum(arrived[...], axis=0)
        target[me] = source[...]
        broadcast(source, target, kind)

    def whole(arrived):
        matrix = jnp.concatenate([arrived[part] for part in range(n)], axis=0)
        if fold == 2:
            return jnp.concatenate([matrix[:, :rank], matrix[:, rank:]], axis=0)
        return matrix[:, :rank]

    barrier = pltpu.get_barrier_semaphore()
    each_peer(
        lambda peer: pl.semaphore_signal(
            barrier, inc=1, device_id={"row": peer}, device_id_type=MESH
        )
    )

    def load_table(source, target, kind):
        return [
            pltpu.make_async_copy(
                source.at[:, pl.ds(part * width, width)],
                target.at[pl.ds(part * rank, rank)],
                load_sems.at[kind],
            )
            for part in range(source.shape[1] // width)
        ]

    def load(source, target, kind):
        return [pltpu.make_async_copy(source, target, load_sems.at[kind])]

    loads = [
        load(k_hbm, k_ref, 0) + load_table(c_hbm, folded_c, 0),
        load(count_hbm, count_ref, 1)
        + load(values_hbm, values_ref, 1)
        + load(sample_hbm, sample_ref, 1),
        load(j_hbm, j_ref, 2) + load(w_hbm, w_ref, 2) + load_table(b_hbm, folded_b, 2),
    ]
    for copies in loads:
        for copy in copies:
            copy.start()

    def loaded(kind):
        for copy in loads[kind]:
            copy.wait()

    def pick_c(peer):
        return pick_columns(folded_c, k_ref[peer] - me * c_rows, rank).astype(jnp.bfloat16)

    loaded(0)
    c_out[send_turn(0)] = pick_c(send_turn(0))
    loaded(1)
    lanes = lax.broadcasted_iota(jnp.int32, (blocks, 128), 1)
    counts = block_column(count_ref)
    live = lanes < counts
    masked = jnp.where(live, values_ref[...].astype(jnp.float32), 0.0).astype(jnp.bfloat16)
    values_out[...] = masked.reshape(values_out.shape)
    values_in[me] = values_out[me]
    live_local = jnp.sum(counts.astype(jnp.float32), axis=0, keepdims=True)
    pl.semaphore_wait(barrier, n - 1)
    copy_c(send_turn(0), me).start()

    def send_c(peer):
        c_out[peer] = pick_c(peer)
        copy_c(peer, me).start()

    def send_far(turn, carry):
        send_c(send_turn(turn))
        return carry

    def send_near(turn, carry):
        send_c(sibling(turn))
        return carry

    lax.fori_loop(1, 3 * quarter, send_far, 0)
    lax.fori_loop(1, quarter, send_near, 0)

    @pl.when(inner == 1)
    def _():
        spread_out(values_out, values_in, 0)

    c_in[me] = pick_c(me)
    loaded(2)

    def pick_b(part, carry):
        picked = pick_columns(folded_b, j_ref[part] - me * b_rows, rank)
        b_weighted[part] = w_ref[part] * picked
        return carry

    lax.fori_loop(0, n, pick_b, 0)
    columns = lax.broadcasted_iota(jnp.int32, (blocks, chunk), 1)
    sample_column[...] = block_column(sample_ref)

    def add_chunk(part, carry):
        gram, picks = carry
        weights = w_ref[part]
        sketch = b_weighted[part] * c_in[part].astype(jnp.float32)
        both = jnp.concatenate(halves(sketch), axis=0)
        gram = gram + lax.dot_general(both, both, NT, preferred_element_type=jnp.float32)
        weighted = (weights * sketch).astype(jnp.bfloat16)
        chosen = columns == sample_column[...] - part * chunk
        chosen = jnp.where(chosen, 1.0, 0.0).astype(jnp.bfloat16)
        picks = picks + lax.dot_general(
            chosen, weighted, NT, preferred_element_type=jnp.float32
        )
        return gram, picks

    def add_peer(part, carry):
        copy_c(part, part).wait_recv()
        return add_chunk(part, carry)

    carry = (
        jnp.zeros((2 * rank, 2 * rank), jnp.float32),
        jnp.zeros((blocks, rank), jnp.float32),
    )
    carry = add_chunk(me, carry)
    carry = lax.fori_loop(
        0, quarter, lambda turn, carry: add_peer(member(1 + 2 * inner, quarter - turn), carry), carry
    )
    carry = lax.fori_loop(
        1, quarter, lambda turn, carry: add_peer(sibling(quarter - turn), carry), carry
    )

    def add_late(turn, carry):
        carry = add_peer(late_turn(turn), carry)

        @pl.when((inner == 1) & (turn == 3 * quarter // 2 - 1))
        def _():
            pl.semaphore_signal(
                turn_sem, inc=1, device_id={"row": member(0, 0)}, device_id_type=MESH
            )

        return carry

    gram, picks = lax.fori_loop(0, 2 * quarter, add_late, carry)

    @pl.when(inner == 0)
    def _():
        pl.semaphore_wait(turn_sem, 1)
        spread_out(values_out, values_in, 0)

    pair = gram[:rank] + gram[rank:]
    pair = (pair + pltpu.roll(pair, rank, 1)) / total_samples
    pair_rows = lax.broadcasted_iota(jnp.int32, pair.shape, 0)
    pair_lanes = lax.broadcasted_iota(jnp.int32, pair.shape, 1)
    ridge = 0.05 * live_local / total_rows
    pair = pair + jnp.where(pair_lanes % rank == pair_rows, ridge, 0.0)
    scatter(pair, gram_out, gram_in, 1)

    rows_half = per_peer // 2
    picks = picks.reshape(n, per_peer, rank)
    picks_out[...] = jnp.concatenate(
        [picks[:, :rows_half], picks[:, rows_half:]], axis=2
    ).astype(jnp.bfloat16)
    picks_in[me] = picks_out[me]
    spread_out(picks_out, picks_in, 2)

    others(0, values_in).wait_recv()
    arrived = values_in[...].astype(jnp.float32)
    tile_of = lax.broadcasted_iota(jnp.int32, (n * rows_half, 128), 0) % rows_half // slots
    for part in range(2):
        rows = arrived[:, part * rows_half : (part + 1) * rows_half, :].reshape(-1, 128)
        spread_ref[part] = jnp.concatenate(
            [jnp.where(tile_of == tile, rows, 0.0) for tile in range(tiles // 2)], axis=1
        ).astype(jnp.bfloat16)

    others(1, gram_in).wait_recv()
    gather(gram_in, share_out, share_in, 3)
    others(2, picks_in).wait_recv()
    arrived = picks_in[...].astype(jnp.float32).reshape(-1, 2 * rank).astype(jnp.bfloat16)
    gathered = jnp.concatenate(
        [
            lax.dot_general(arrived, spread_ref[part], TN, preferred_element_type=jnp.float32)[
                part * rank : (part + 1) * rank
            ]
            for part in range(2)
        ],
        axis=1,
    )
    part = rank // 2
    split = halves(gathered)
    columns = [jnp.concatenate([x] * 2 + [x[part:]] * 4, axis=0) for x in split]
    split = jnp.concatenate(split, axis=0)
    moments = sum(
        lax.dot_general(split, x, NT, preferred_element_type=jnp.float32) for x in columns
    )
    moments = moments[:rank] + moments[rank:]
    top, low = moments[:part, : 2 * rank], moments[part:, 2 * rank :]
    rows = lax.broadcasted_iota(jnp.int32, (part, 2 * rank), 0)
    lanes = lax.broadcasted_iota(jnp.int32, (part, 2 * rank), 1)
    across = lanes % rank
    triangle = jnp.where(across >= rows, jnp.where(across == rows, top, 2.0 * top), 2.0 * low)
    quarter_rows = part // 2
    moment_out[:quarter_rows] = jnp.where(
        lanes[:quarter_rows] < rank, triangle[:quarter_rows], triangle[quarter_rows:]
    )
    moment_out[quarter_rows:] = jnp.sum(
        jnp.where(lanes == rows, low, 0.0), axis=0, keepdims=True
    )
    moment_in[me] = moment_out[...]
    broadcast(moment_out, moment_in, 4)

    others(3, share_in).wait_recv()
    inverted = inverse(whole(share_in))
    first = jnp.concatenate([inverted] * 2, axis=1)
    second = jnp.concatenate([inverted[:, part:]] * 4, axis=1)
    others(4, moment_in).wait_recv()
    moment = jnp.sum(moment_in[...], axis=0)
    triangle, corner = moment[:quarter_rows], moment[quarter_rows:]
    above = across >= rows
    stacked = jnp.concatenate([triangle] * 2, axis=0)
    stacked = jnp.where((lanes < rank) == (rows < quarter_rows), stacked, 0.0)
    zeros = jnp.zeros_like(stacked)
    stacked = jnp.concatenate(
        [
            jnp.concatenate([jnp.where(above, stacked, 0.0), zeros], axis=1),
            jnp.concatenate([zeros, jnp.where(above, 0.0, stacked)], axis=1),
        ],
        axis=0,
    )
    both = product(inverted, jnp.concatenate([stacked, gathered], axis=1))
    solved, update_ref[...] = both[:, : 4 * rank], both[:, 4 * rank :]
    squares = jnp.sum(
        solved[:, : 2 * rank] * first
        + solved[:, 2 * rank :] * second
        + corner * second * second,
        axis=1,
        keepdims=True,
    )
    squares_ref[...] = squares

    for sent in (c_out, values_out, gram_out, picks_out, share_in, moment_in):
        others(0, sent).wait_send()


def shards(
    factor_b, factor_c, sample_j, sample_k, sample_weight, block_values, block_sample, block_count
):
    rank, b_rows = factor_b.shape
    n, _, chunk = sample_k.shape
    _, _, tiles, slots, tile_rows = block_values.shape
    samples = sample_j.shape[0]
    per_peer = tiles * slots
    blocks = n * per_peer
    width = 512
    piece = max(rank // (2 * n), 1)
    bf16, f32, i32 = jnp.bfloat16, jnp.float32, jnp.int32
    hbm = pl.BlockSpec(memory_space=pltpu.HBM)
    vmem = pl.BlockSpec(memory_space=pltpu.VMEM)
    total_rows = tiles * tile_rows * n
    update, squares = pl.pallas_call(
        functools.partial(kernel, n, tiles, slots, total_rows, samples * n),
        out_shape=(
            pltpu.VMEM((rank, tiles * tile_rows), f32),
            pltpu.VMEM((rank, 1), f32),
        ),
        in_specs=[hbm] * 8,
        out_specs=(vmem, vmem),
        scratch_shapes=[
            pltpu.VMEM((b_rows // width * rank, width), bf16),
            pltpu.VMEM((factor_c.shape[1] // width * rank, width), bf16),
            pltpu.VMEM((n, 1, chunk), i32),
            pltpu.VMEM((n, 1, chunk), i32),
            pltpu.VMEM((n, 1, chunk), f32),
            pltpu.VMEM((blocks, tile_rows), bf16),
            pltpu.VMEM((tiles, slots, n), i32),
            pltpu.VMEM((tiles, slots, n), i32),
            pltpu.VMEM((n, rank, chunk), bf16),
            pltpu.VMEM((n, rank, chunk), bf16),
            pltpu.VMEM((n, rank, chunk), f32),
            pltpu.VMEM((n, per_peer, tile_rows), bf16),
            pltpu.VMEM((n, per_peer, tile_rows), bf16),
            pltpu.VMEM((2, blocks // 2, tiles // 2 * tile_rows), bf16),
            pltpu.VMEM((n, per_peer // 2, 2 * rank), bf16),
            pltpu.VMEM((n, per_peer // 2, 2 * rank), bf16),
            pltpu.VMEM((n, piece, 2 * rank), f32),
            pltpu.VMEM((n, piece, 2 * rank), f32),
            pltpu.VMEM((piece, 2 * rank), f32),
            pltpu.VMEM((n, piece, 2 * rank), f32),
            pltpu.VMEM((blocks, 1), i32),
            pltpu.VMEM((rank // 4 + 1, 2 * rank), f32),
            pltpu.VMEM((n, rank // 4 + 1, 2 * rank), f32),
            pltpu.SemaphoreType.DMA((3,)),
            pltpu.SemaphoreType.DMA((n,)),
            pltpu.SemaphoreType.DMA,
            pltpu.SemaphoreType.DMA((5,)),
            pltpu.SemaphoreType.REGULAR,
        ],
        compiler_params=pltpu.CompilerParams(collective_id=0, has_side_effects=True),
    )(
        factor_b,
        factor_c,
        sample_j.reshape(n, 1, chunk),
        sample_k,
        sample_weight.reshape(n, 1, chunk),
        block_values.reshape(blocks, tile_rows),
        block_sample[0].transpose(1, 2, 0),
        block_count[0].transpose(1, 2, 0),
    )
    scales = jnp.sqrt(jnp.maximum(squares, 0.0) / total_rows + 1e-06)
    return (update / scales).astype(bf16), scales.reshape(rank)


def solution(mesh):
    in_specs = (
        P(None, ("groups", "row")),
        P(None, ("groups", "row")),
        P(("groups", "row")),
        P(None, ("groups", "row"), None),
        P(("groups", "row")),
        P(("groups", "row"), None, None, None, None),
        P(("groups", "row"), None, None, None),
        P(("groups", "row"), None, None, None),
    )
    out_specs = (P(None, ("groups", "row")), P("groups"))
    return jax.shard_map(shards, mesh=mesh, in_specs=in_specs, out_specs=out_specs, check_vma=False)
```
